32 devices in a mesh: depth: 8 (over y, x, core), image: 4 (over z).
Axes of the slice: x: 2, y: 2, z: 4, core: 2. Of those that a mesh axis runs over, the one named last changes fastest.
Arguments:
- bricks: bfloat16 [8, 1024, 16, 256], P('depth', 'image'), may hold values from -6 to 6
- cost: int32 [8, 1024], P('depth', 'image'), may hold values from 0 to 4, as said below
- order: int32 [2, 8], replicated, may hold values from 0 to 7, as said below
- color_gain: float32 [3], replicated, may hold values from 0.5 to 2
- color_bias: float32 [3], replicated, may hold values from -1 to 1
- ext_gain: float32 [1], replicated, may hold values from 0.6 to 1.4
- ext_bias: float32 [1], replicated, may hold values from -4.6 to -3.6
Outputs:
- frames: float32 [2, 4, 256, 1024], P(None, None, 'depth', 'image')
The draws below stay inside these ranges and needn't reach their ends.
Inputs may be any that keep to these rules, and one draw needn't show every extreme that they name: In each slab the 4 tiles hold together exactly 512 bricks of cost above 0, and one tile of each slab has all 256 of its bricks nonempty. `order`: row v holds, for slab s, the bitwise exclusive or of s with a number m_v of 0 to 8 - 1 (the same for the whole row).
All inputs are finite; a program needn't handle non-finite values.
Results may differ from the reference program's by a relative error of at most 0.0003.
Values may be sent and summed in bfloat16 or wider, within the bound.
No kernel may reach another device: no remote copies, remote signals or barrier semaphores. Data moves between devices by JAX's collectives and lax.ppermute only.
A program may use at most 128 MiB of HBM per device.

```python
import jax
import jax.numpy as jnp
from jax import lax

BE = 16
BC = 16
NB = 256
TR = 256
TC = 256
N_DEPTH = 8
N_IMAGE = 4


def draw_cost(key, part):

    def one_slab(slab_key):
        key_full, key_weight, key_perm, key_level = jax.random.split(slab_key, 4)
        places = jnp.arange(N_IMAGE, dtype=jnp.int32)
        full_tile = jax.random.randint(key_full, (), 0, N_IMAGE)
        weights = jax.random.randint(key_weight, (N_IMAGE,), 2, 5)
        weights = jnp.where(places == full_tile, 0, weights)
        spread_total = NB * (N_IMAGE // 2 - 1)
        shares = weights * spread_total // jnp.sum(weights)
        shortfall = spread_total - jnp.sum(shares)
        distance = (places - full_tile - 1) % N_IMAGE
        shares = shares + (distance < shortfall).astype(jnp.int32)
        counts = jnp.where(places == full_tile, NB, shares)
        perm_keys = jax.random.split(key_perm, N_IMAGE)
        ranks = jax.vmap(lambda one_key: jax.random.permutation(one_key, NB))(perm_keys)
        levels = jax.random.randint(key_level, (N_IMAGE, NB), 1, 5)
        return jnp.where(ranks < counts[:, None], levels, 0).reshape(N_IMAGE * NB)
    slab_keys = jax.random.split(jax.random.fold_in(key, 11), N_DEPTH)
    return jax.vmap(one_slab)(slab_keys).astype(jnp.int32)


def draw_order(key, part):
    masks = jax.random.randint(jax.random.fold_in(key, 23), (2, 1), 0, N_DEPTH).astype(jnp.int32)
    slab_index = jnp.arange(N_DEPTH, dtype=jnp.int32)[None, :]
    return jnp.bitwise_xor(slab_index, masks).astype(jnp.int32)


def block_scale(rng, shape, cuts, least, largest):
    def one(dim, parts):
        heights = jax.random.uniform(jax.random.fold_in(jax.random.fold_in(rng, 6), dim), (parts,), jnp.float32, least / len(cuts), largest / len(cuts))
        return jnp.repeat(jnp.exp(heights), shape[dim] // parts).reshape((-1,) + (1,) * (len(shape) - dim - 1))

    loudness = one(*cuts[0])
    for cut in cuts[1:]:
        loudness = loudness * one(*cut)
    return loudness


def bell_draw(stream_key, dims, width, bound, cuts=(), kind=jnp.bfloat16):
    drawn = jax.random.normal(stream_key, dims, jnp.float32) * width
    if len(cuts) > 0:
        drawn = block_scale(stream_key, dims, cuts, -0.22, 0.18) * drawn
    return jnp.clip(drawn, min=-bound, max=bound).astype(kind)


def setup_inputs(seed: int = 0) -> dict:
    key_list = jax.random.split(jax.random.key(seed), 8)
    bricks = bell_draw(key_list[0], (N_DEPTH, NB * N_IMAGE, BE, BE * BE), 1.0, 6.0, ((0, 8), (1, 4)))
    cost = draw_cost(jax.random.fold_in(key_list[7], 71), 0)
    order = draw_order(jax.random.fold_in(key_list[7], 71), 0)
    color_gain = jnp.clip(jax.random.uniform(key_list[3], (3,), jnp.float32, 0.5, 2.0), 0.5, 2.0)
    color_bias = jnp.clip(jax.random.uniform(key_list[4], (3,), jnp.float32, -1.0, 1.0), -1.0, 1.0)
    ext_gain = jnp.clip(jax.random.uniform(key_list[5], (1,), jnp.float32, 0.6, 1.4), 0.6, 1.4)
    ext_bias = jnp.clip(jax.random.uniform(key_list[6], (1,), jnp.float32, -4.6, -3.6), -4.6, -3.6)
    return {"bricks": bricks, "cost": cost, "order": order, "color_gain": color_gain, "color_bias": color_bias, "ext_gain": ext_gain, "ext_bias": ext_bias}


SHEAR = (0.45, -0.3)


def shear_taps(brick_edge, view):
    slice_index = jnp.arange(brick_edge, dtype=jnp.float32)[:, None]
    position = jnp.arange(brick_edge, dtype=jnp.float32)[None, :] + SHEAR[view] * (slice_index - (brick_edge - 1) / 2.0)
    anchor = jnp.floor(position)
    fraction = position - anchor
    weight_low = lax.optimization_barrier((1.0 - fraction).astype(jnp.bfloat16)).astype(jnp.float32)
    weight_high = lax.optimization_barrier(fraction.astype(jnp.bfloat16)).astype(jnp.float32)
    return anchor.astype(jnp.int32), weight_low, weight_high


def shade_samples(samples, levels, flip, color_gain, color_bias, ext_gain, ext_bias):
    brick_edge = samples.shape[1]
    slice_index = jnp.arange(brick_edge, dtype=jnp.int32)
    occupied = (slice_index[None, :] * 4 < levels[:, None] * brick_edge).astype(samples.dtype)[:, :, None]
    samples = jnp.where(flip, samples[:, ::-1], samples)
    occupied = jnp.where(flip, occupied[:, ::-1], occupied)
    extinction = jnp.exp(ext_gain[0] * samples + ext_bias[0])
    opacity = (1.0 - jnp.exp(-extinction)) * occupied
    remaining = jnp.cumprod(1.0 - opacity, axis=1)
    ahead_clear = jnp.concatenate([jnp.ones_like(remaining[:, :1]), remaining[:, :-1]], axis=1)
    weight = ahead_clear * opacity
    colors = [jnp.sum(weight * jax.nn.sigmoid(color_gain[channel] * samples + color_bias[channel]), axis=1) for channel in range(3)]
    return jnp.stack(colors + [1.0 - remaining[:, -1]], axis=1)


def sample_view(density, view):
    total_bricks, brick_edge, plane_size = density.shape
    voxels = density.reshape(total_bricks, brick_edge, brick_edge, brick_edge)
    anchor, weight_low, weight_high = shear_taps(brick_edge, view)

    def spread(table):
        if view == 0:
            return table[None, :, None, :]
        return table[None, :, :, None]

    def fetch_taps(indices):
        inside = ((indices >= 0) & (indices < brick_edge)).astype(density.dtype)
        clipped = jnp.clip(indices, 0, brick_edge - 1).astype(jnp.int32)
        values = jnp.take_along_axis(voxels, jnp.broadcast_to(spread(clipped), voxels.shape), axis=3 if view == 0 else 2)
        return values * spread(inside)

    samples = fetch_taps(anchor) * spread(weight_low) + fetch_taps(anchor + 1) * spread(weight_high)
    return samples.reshape(total_bricks, brick_edge, plane_size)


def arrange_tile(segments):
    brick_edge = BE
    rows = segments.shape[0] // BC
    tile_image = segments.reshape(rows, BC, 2, 4, brick_edge, brick_edge)
    tile_image = tile_image.transpose(2, 3, 0, 4, 1, 5)
    return tile_image.reshape(2, 4, rows * brick_edge, BC * brick_edge)


def composite(front_part, back_part):
    return front_part + (1.0 - front_part[..., 3:4, :, :]) * back_part


def reference(bricks, cost, order, color_gain, color_bias, ext_gain, ext_bias):
    flips = order[:, 0] > order[:, -1]
    by_rank = jnp.argsort(order, axis=1).astype(jnp.int32)
    zero_index = jnp.zeros((), jnp.int32)

    def one_tile(tile_number):
        offset = (tile_number * NB).astype(jnp.int32)

        def advance(totals, position):
            layers = []
            for view in range(2):
                slab_index = by_rank[view, position]
                density = lax.dynamic_slice(bricks, (slab_index, offset, zero_index, zero_index), (1, NB, BE, BE * BE))[0].astype(jnp.float32)
                levels = lax.dynamic_slice(cost, (slab_index, offset), (1, NB))[0]
                layers.append(shade_samples(sample_view(density, view), levels, flips[view], color_gain, color_bias, ext_gain, ext_bias))
            tile_image = arrange_tile(jnp.stack(layers, axis=1))
            return composite(totals, tile_image), None

        start = jnp.zeros((2, 4, TR, TC), jnp.float32)
        totals, unused = lax.scan(advance, start, jnp.arange(N_DEPTH, dtype=jnp.int32))
        return totals

    tiles = lax.map(one_tile, jnp.arange(N_IMAGE, dtype=jnp.int32))
    return tiles.transpose(1, 2, 3, 0, 4).reshape(2, 4, TR, N_IMAGE * TC)
```

```python
import functools
import math

import jax
import jax.numpy as jnp
import numpy as np
from jax import lax
from jax.experimental import pallas as pl
from jax.experimental.pallas import tpu as pltpu
from jax.sharding import PartitionSpec as P

BC = 16
LANES = 128
SUB = 8
SHEAR = (0.45, -0.3)
LOG2E = 1.0 / math.log(2.0)

CODE_RANGE = 32.0
CODE_STEP = 2047.0
CODE_BIAS = 32768.0


def shear_taps(brick_edge, view):
    f32 = np.float32
    slice_index = np.arange(brick_edge, dtype=f32)[:, None]
    position = np.arange(brick_edge, dtype=f32)[None, :] + f32(SHEAR[view]) * (
        slice_index - f32((brick_edge - 1) / 2.0)
    )
    anchor = np.floor(position)
    fraction = (position - anchor).astype(f32)
    low = (f32(1.0) - fraction).astype(jnp.bfloat16).astype(f32)
    high = fraction.astype(jnp.bfloat16).astype(f32)
    return anchor.astype(np.int32), low, high


def shear_lines(brick_edge, view):
    anchor, low, high = shear_taps(brick_edge, view)
    source = np.arange(brick_edge)[None, :, None]
    table = np.where(source == anchor[:, None, :], low[:, None, :], 0.0)
    return table + np.where(source == anchor[:, None, :] + 1, high[:, None, :], 0.0)


def shear_tables(edge):
    along_cols = shear_lines(edge, 0)
    along_rows = shear_lines(edge, 1)
    block = np.stack([np.kron(np.eye(LANES // edge), t) for t in along_cols])
    full = np.stack([np.kron(t, np.eye(edge)) for t in along_rows])
    lane = np.arange(LANES)
    turned = (-(lane // edge) % (LANES // edge)) * edge + lane % edge
    block = block[:, :, turned]
    full = full.reshape(edge, edge * edge, -1, LANES)[..., turned].reshape(full.shape)
    return block.astype(jnp.bfloat16), full.astype(jnp.bfloat16)


def encode(x):
    logs = jnp.log(jnp.maximum(x, 2.0**-CODE_RANGE))
    code = logs * (CODE_STEP * LOG2E) + (CODE_RANGE * CODE_STEP + 0.5)
    return (code.astype(jnp.int32) - int(CODE_BIAS)).astype(jnp.int16)


def decode(code):
    value = code.astype(jnp.int32).astype(jnp.float32)
    return jnp.exp2(value * (1.0 / CODE_STEP) + (CODE_BIAS / CODE_STEP - CODE_RANGE))


def bit_of(value, bit):
    return lax.bitwise_and(lax.shift_right_logical(value, bit), 1)


def spread_bit(slot, position, bit):
    high = lax.shift_left(lax.shift_right_logical(slot, position), position + 1)
    low = lax.bitwise_and(slot, (1 << position) - 1)
    return high + low + bit * (1 << position)


def render_kernel(
    rounds, keep, low_bits, edge,
    order, cgain, cbias, egain, ebias, cost, bricks, table0, table1,
    out_send, out_keep,
    xin, tab0, tab1, moved, samples, perm, levels, sems,
):
    me = lax.axis_index("depth")
    rows, slabs = xin.shape[0], order.shape[1]
    chunk_bricks = rows * BC
    plane = edge * edge
    halves = plane // LANES
    top = bit_of(me, rounds - 1)
    half = top if keep else 1 - top
    first = half * chunk_bricks

    copies = []
    for r in range(rows):
        copies.append(
            pltpu.make_async_copy(bricks.at[pl.ds(first + r * BC, BC)], xin.at[r], sems.at[r])
        )
    for h in range(halves):
        span = pl.ds(h * LANES, LANES)
        copies.append(pltpu.make_async_copy(table0, tab0.at[:, span, span], sems.at[rows + h]))
    copies.append(pltpu.make_async_copy(table1, tab1, sems.at[rows + halves]))
    for copy in copies:
        copy.start()

    size = BC * edge
    out_row = lax.broadcasted_iota(jnp.int32, (size, size), 0)
    in_row = lax.broadcasted_iota(jnp.int32, (size, size), 1)
    wanted = lax.rem(out_row, BC) * edge + out_row // BC
    perm[...] = jnp.where(wanted == in_row, 1.0, 0.0).astype(jnp.bfloat16)

    here = lax.broadcasted_iota(jnp.int32, (chunk_bricks, chunk_bricks), 0)
    there = lax.broadcasted_iota(jnp.int32, (chunk_bricks, chunk_bricks), 1)
    cost_row = jnp.where(
        half == 0, cost[0:1, :chunk_bricks], cost[0:1, chunk_bricks:]
    ).astype(jnp.float32)
    picked = jnp.where(here == there, cost_row, 0.0).astype(jnp.bfloat16)
    levels[...] = jnp.dot(
        picked, jnp.ones((chunk_bricks, LANES), jnp.bfloat16), preferred_element_type=jnp.float32
    )

    zero = jnp.zeros((LANES, LANES), jnp.bfloat16)
    for k in range(edge):
        for a in range(halves):
            for b in range(halves):
                if a != b:
                    tab0[k, a * LANES : (a + 1) * LANES, b * LANES : (b + 1) * LANES] = zero

    for r in range(rows):
        copies[r].wait()
        line = xin[r].reshape(size, plane)
        slices = jnp.dot(perm[...], line, preferred_element_type=jnp.float32).astype(jnp.bfloat16)
        for k in range(edge):
            moved[k, r * BC : (r + 1) * BC, :] = slices[k * BC : (k + 1) * BC, :]

    flips = [order[v, 0] > order[v, slabs - 1] for v in range(2)]

    def resample(v, k):
        table = tab0 if v == 0 else tab1
        result = jnp.dot(moved[k], table[k], preferred_element_type=jnp.float32)
        place = jnp.where(flips[v], edge - 1 - k, k)
        for h in range(halves):
            samples[v, place, h] = result[:, h * LANES : (h + 1) * LANES]

    ext_slope = egain[0] * LOG2E
    ext_shift = ebias[0] * LOG2E + math.log2(LOG2E)
    slopes = [cgain[c] * 0.5 for c in range(3)]
    shifts = [cbias[c] * 0.5 for c in range(3)]
    mine = bit_of(me, 0)
    per_kind = chunk_bricks // SUB * halves // 2
    per_level = edge // 4

    def shade(v, item, kind, out):
        slot, group = item // 2, lax.rem(item, 2)
        unit = spread_bit(slot, low_bits, mine if kind == 0 else 1 - mine)
        h = lax.rem(unit, halves)
        start = pl.multiple_of((unit // halves) * BC + group * SUB, SUB)
        level = levels[pl.ds(start, SUB), :]
        shift = []
        for j in range(4):
            need = jnp.where(flips[v], 3 - j, j).astype(jnp.float32)
            shift.append(jnp.where(level > need, ext_shift, -1e30))
        clear = jnp.ones((SUB, LANES), jnp.float32)
        sums = [jnp.zeros((SUB, LANES), jnp.float32) for _ in range(3)]
        for k in range(edge):
            s = samples[v, k, h, pl.ds(start, SUB), :]
            passed = jnp.exp2(-jnp.exp2(s * ext_slope + shift[k // per_level]))
            beyond = clear * passed
            weight = clear - beyond
            clear = beyond
            for c in range(3):
                sums[c] = sums[c] + weight * jnp.tanh(s * slopes[c] + shifts[c])
        opacity = 1.0 - clear
        place = pl.multiple_of(group * SUB, SUB)
        for c in range(3):
            out[slot, v, c, pl.ds(place, SUB), :] = (opacity + sums[c]) * 0.5
        out[slot, v, 3, pl.ds(place, SUB), :] = opacity

    for h in range(halves):
        copies[rows + h].wait()
    for k in range(edge):
        resample(0, k)
    copies[rows + halves].wait()

    def both(i, carry):
        resample(1, i)
        for kind, out in ((1, out_send), (0, out_keep)):
            for n in range(per_kind // edge):
                shade(0, i * (per_kind // edge) + n, kind, out)
        return carry

    lax.fori_loop(0, edge, both, 0)

    def last(i, carry):
        for kind, out in ((1, out_send), (0, out_keep)):
            shade(1, i, kind, out)
        return carry

    lax.fori_loop(0, per_kind, last, 0)


def render(rounds, keep, low_bits, scalars, cost, bricks, table0, table1):
    total, edge, plane = bricks.shape
    rows = total // BC // 2
    chunk = rows * BC
    halves = plane // LANES
    units = rows * halves
    shape = jax.ShapeDtypeStruct((units // 2, 2, 4, BC, LANES), jnp.float32)
    smem = pl.BlockSpec(memory_space=pltpu.SMEM)
    vmem = pl.BlockSpec(memory_space=pltpu.VMEM)
    hbm = pl.BlockSpec(memory_space=pl.ANY)
    return pl.pallas_call(
        functools.partial(render_kernel, rounds, keep, low_bits, edge),
        out_shape=(shape, shape),
        in_specs=[smem] * 5 + [vmem, hbm, hbm, hbm],
        out_specs=(vmem, vmem),
        scratch_shapes=[
            pltpu.VMEM((rows, BC, edge, plane), jnp.bfloat16),
            pltpu.VMEM((edge, plane, plane), jnp.bfloat16),
            pltpu.VMEM((edge, plane, plane), jnp.bfloat16),
            pltpu.VMEM((edge, chunk, plane), jnp.bfloat16),
            pltpu.VMEM((2, edge, halves, chunk, LANES), jnp.float32),
            pltpu.VMEM((BC * edge, BC * edge), jnp.bfloat16),
            pltpu.VMEM((chunk, LANES), jnp.float32),
            pltpu.SemaphoreType.DMA((rows + halves + 1,)),
        ],
        compiler_params=pltpu.CompilerParams(vmem_limit_bytes=32 << 20),
        cost_estimate=pl.CostEstimate(
            flops=int(4e6), bytes_accessed=4 << 20, transcendentals=chunk * edge * plane * 10
        ),
        name="render",
    )(*scalars, cost, bricks, table0, table1)


def merged_pair(front_bit, kept, incoming):
    behind = 1.0 - front_bit * incoming[3]
    ahead = 1.0 - (1.0 - front_bit) * kept[3]
    return [kept[c] * behind + incoming[c] * ahead for c in range(4)]


def merge_kernel(bit, low_bits, mode, order, kept, incoming, *outs):
    me = lax.axis_index("depth")
    coded = incoming.dtype == jnp.int16
    units = kept.shape[0]
    mine = bit_of(me, bit + 1)
    for v in range(2):
        front = bit_of(lax.bitwise_xor(me, order[v, 0]), bit).astype(jnp.float32)

        def one(slot, kind, out):
            unit = slot if kind is None else spread_bit(slot, low_bits, mine if kind == 0 else 1 - mine)
            came = [incoming[unit, v, c] for c in range(4)]
            if coded:
                came = [decode(x) for x in came]
            done = merged_pair(front, [kept[unit, v, c] for c in range(4)], came)
            for c in range(4):
                out[slot, v, c] = encode(done[c]) if out.dtype == jnp.int16 else done[c]

        if mode == "split":
            for kind, out in ((1, outs[0]), (0, outs[1])):
                for slot in range(units // 2):
                    one(slot, kind, out)
        else:
            for slot in range(units):
                one(slot, None, outs[0])


def merge(bit, low_bits, mode, order, kept, incoming):
    units = kept.shape[0]
    tail = kept.shape[1:]
    if mode == "split":
        outs = (
            jax.ShapeDtypeStruct((units // 2,) + tail, jnp.int16),
            jax.ShapeDtypeStruct((units // 2,) + tail, jnp.float32),
        )
    elif mode == "send":
        outs = (jax.ShapeDtypeStruct((units,) + tail, jnp.int16),)
    else:
        outs = (jax.ShapeDtypeStruct((units,) + tail, jnp.float32),)
    vmem = pl.BlockSpec(memory_space=pltpu.VMEM)
    return pl.pallas_call(
        functools.partial(merge_kernel, bit, low_bits, mode),
        out_shape=outs,
        in_specs=[pl.BlockSpec(memory_space=pltpu.SMEM), vmem, vmem],
        out_specs=tuple(vmem for _ in outs),
        compiler_params=pltpu.CompilerParams(vmem_limit_bytes=8 << 20),
        cost_estimate=pl.CostEstimate(flops=int(4e5), bytes_accessed=kept.size * 8, transcendentals=0),
        name="merge",
    )(order, kept, incoming)


def finish_kernel(bit, edge, order, kept, incoming, out):
    me = lax.axis_index("depth")
    units = kept.shape[0]
    chunks = LANES // edge
    chunk_of = lax.broadcasted_iota(jnp.int32, (SUB, LANES), 1) // edge
    for v in range(2):
        front = bit_of(lax.bitwise_xor(me, order[v, 0]), bit).astype(jnp.float32)
        for unit in range(units):
            came = [decode(incoming[unit, v, c]) for c in range(4)]
            done = merged_pair(front, [kept[unit, v, c] for c in range(4)], came)
            for c in range(4):
                for g in range(BC // SUB):
                    x = done[c][g * SUB : (g + 1) * SUB, :]
                    x = pltpu.roll(x, 0, 1, stride=edge, stride_axis=0)
                    for step in range(3):
                        turned = pltpu.roll(x, SUB - (1 << step), 0)
                        x = jnp.where(bit_of(chunk_of, step) == 1, turned, x)
                    x = pltpu.roll(x, 0, 1, stride=edge, stride_axis=0)
                    out[v, c, unit * chunks : (unit + 1) * chunks, g * LANES : (g + 1) * LANES] = x


def finish(bit, edge, order, kept, incoming):
    units = kept.shape[0]
    vmem = pl.BlockSpec(memory_space=pltpu.VMEM)
    return pl.pallas_call(
        functools.partial(finish_kernel, bit, edge),
        out_shape=jax.ShapeDtypeStruct((2, 4, units * LANES // edge, BC * edge), jnp.float32),
        in_specs=[pl.BlockSpec(memory_space=pltpu.SMEM), vmem, vmem],
        out_specs=vmem,
        compiler_params=pltpu.CompilerParams(vmem_limit_bytes=8 << 20),
        cost_estimate=pl.CostEstimate(flops=int(4e5), bytes_accessed=kept.size * 8, transcendentals=0),
        name="finish",
    )(order, kept, incoming)


def swapped(x, bit):
    count = lax.axis_size("depth")
    return lax.ppermute(x, "depth", [(i, i ^ 1 << bit) for i in range(count)])


def shards(bricks, cost, order, color_gain, color_bias, ext_gain, ext_bias):
    bricks = bricks[0]
    total, edge, plane = bricks.shape
    count = lax.axis_size("depth")
    rounds = count.bit_length() - 1
    units = total // BC * (plane // LANES)
    low_bits = (units // count).bit_length() - 1
    table0, table1 = (jnp.asarray(t) for t in shear_tables(edge))
    scalars = (order, color_gain, color_bias, ext_gain, ext_bias)

    halves = []
    for keep in (False, True):
        halves.append(render(rounds, keep, low_bits, scalars, cost, bricks, table0, table1))
    parts = []
    for keep, (send, kept) in zip((False, True), halves):
        for bit in range(rounds - 1):
            incoming = swapped(send, bit)
            if bit < rounds - 2:
                send, kept = merge(bit, low_bits, "split", order, kept, incoming)
            else:
                (done,) = merge(bit, low_bits, "keep" if keep else "send", order, kept, incoming)
        parts.append(done)
    incoming = swapped(parts[0], rounds - 1)
    return finish(rounds - 1, edge, order, parts[1], incoming)


def solution(mesh):
    in_specs = (P("depth", "image", None, None), P("depth", "image"), P(), P(), P(), P(), P())
    out_specs = P(None, None, "depth", "image")
    return jax.shard_map(shards, mesh=mesh, in_specs=in_specs, out_specs=out_specs, check_vma=False)
```

```python
import functools
import math

import jax
import jax.numpy as jnp
import numpy as np
from jax import lax
from jax.experimental import pallas as pl
from jax.experimental.pallas import tpu as pltpu
from jax.sharding import PartitionSpec as P

BC = 16
LANES = 128
SUB = 8
SHEAR = (0.45, -0.3)
LOG2E = 1.0 / math.log(2.0)

CODE_RANGE = 32.0
CODE_STEP = 2047.0
CODE_BIAS = 32768.0


def shear_taps(brick_edge, view):
    f32 = np.float32
    slice_index = np.arange(brick_edge, dtype=f32)[:, None]
    position = np.arange(brick_edge, dtype=f32)[None, :] + f32(SHEAR[view]) * (
        slice_index - f32((brick_edge - 1) / 2.0)
    )
    anchor = np.floor(position)
    fraction = (position - anchor).astype(f32)
    low = (f32(1.0) - fraction).astype(jnp.bfloat16).astype(f32)
    high = fraction.astype(jnp.bfloat16).astype(f32)
    return anchor.astype(np.int32), low, high


def shear_lines(brick_edge, view):
    anchor, low, high = shear_taps(brick_edge, view)
    source = np.arange(brick_edge)[None, :, None]
    table = np.where(source == anchor[:, None, :], low[:, None, :], 0.0)
    return table + np.where(source == anchor[:, None, :] + 1, high[:, None, :], 0.0)


def shear_tables(edge):
    along_cols = shear_lines(edge, 0)
    along_rows = shear_lines(edge, 1)
    block = np.stack([np.kron(np.eye(LANES // edge), t) for t in along_cols])
    full = np.stack([np.kron(t, np.eye(edge)) for t in along_rows])
    lane = np.arange(LANES)
    turned = (-(lane // edge) % (LANES // edge)) * edge + lane % edge
    block = block[:, :, turned]
    full = full.reshape(edge, edge * edge, -1, LANES)[..., turned].reshape(full.shape)
    return block.astype(jnp.bfloat16), full.astype(jnp.bfloat16)


def encode(x):
    logs = jnp.log(jnp.maximum(x, 2.0**-CODE_RANGE))
    code = logs * (CODE_STEP * LOG2E) + (CODE_RANGE * CODE_STEP + 0.5)
    return (code.astype(jnp.int32) - int(CODE_BIAS)).astype(jnp.int16)


def decode(code):
    value = code.astype(jnp.int32).astype(jnp.float32)
    return jnp.exp2(value * (1.0 / CODE_STEP) + (CODE_BIAS / CODE_STEP - CODE_RANGE))


EXT_SLOPE, EXT_SHIFT, SLOPES, SHIFTS, FLIPS, FRONTS = 0, 1, 2, 5, 8, 10


def bit_of(value, bit):
    return lax.bitwise_and(lax.shift_right_logical(value, bit), 1)


def spread_bit(slot, position, bit):
    high = lax.shift_left(lax.shift_right_logical(slot, position), position + 1)
    low = lax.bitwise_and(slot, (1 << position) - 1)
    return high + low + bit * (1 << position)


def shade(item, bit, low_bits, v, samples, levels, splats, out):
    edge, halves = samples.shape[0], samples.shape[1]
    slot, group = item // 2, lax.rem(item, 2)
    unit = spread_bit(slot, low_bits, bit)
    h = lax.rem(unit, halves)
    start = pl.multiple_of((unit // halves) * BC + group * SUB, SUB)
    level = levels[pl.ds(start, SUB), :]
    flip = splats[FLIPS + v]
    ext_slope, ext_shift = splats[EXT_SLOPE], splats[EXT_SHIFT]
    shift = []
    for j in range(4):
        need = j + flip * (3 - 2 * j)
        shift.append(jnp.where(level > need, ext_shift, -1e30))
    clear = jnp.ones((SUB, LANES), jnp.float32)
    sums = [jnp.zeros((SUB, LANES), jnp.float32) for _ in range(3)]
    for k in range(edge):
        s = samples[k, h, pl.ds(start, SUB), :]
        passed = jnp.exp2(-jnp.exp2(s * ext_slope + shift[k // (edge // 4)]))
        beyond = clear * passed
        weight = clear - beyond
        clear = beyond
        for c in range(3):
            sums[c] = sums[c] + weight * jnp.tanh(s * splats[SLOPES + c] + splats[SHIFTS + c])
    opacity = 1.0 - clear
    place = pl.multiple_of(group * SUB, SUB)
    for c in range(3):
        out[slot, c, pl.ds(place, SUB), :] = (opacity + sums[c]) * 0.5
    out[slot, 3, pl.ds(place, SUB), :] = opacity


def shade_pair(i, low_bits, v, samples, levels, splats, send, kept):
    mine = bit_of(lax.axis_index("depth"), 0)
    shade(i, 1 - mine, low_bits, v, samples, levels, splats, send)
    shade(i, mine, low_bits, v, samples, levels, splats, kept)


def to_slices(lines, r, perm, moved):
    edge = moved.shape[0]
    x = lines[r].reshape(BC * edge, lines.shape[-1])
    slices = jnp.dot(perm[...], x, preferred_element_type=jnp.float32).astype(jnp.bfloat16)
    for k in range(edge):
        place = r * BC if isinstance(r, int) else pl.multiple_of(r * BC, BC)
        moved[k, pl.ds(place, BC), :] = slices[k * BC : (k + 1) * BC, :]


def resample(k, v, moved, table, splats, samples):
    edge, halves = samples.shape[0], samples.shape[1]
    result = jnp.dot(moved[k], table[k], preferred_element_type=jnp.float32)
    flip = splats[FLIPS + v, 0, 0] > 0.5
    place = jnp.where(flip, edge - 1 - k, k)
    for h in range(halves):
        samples[place, h] = result[:, h * LANES : (h + 1) * LANES]


def first_kernel(
    rounds, low_bits,
    order, cgain, cbias, egain, ebias, cost, bricks, table0, table1,
    send, kept, next_samples, next_lines, tab0, tab1, perm, levels, splats,
    lines, moved, samples, s_order, s_cgain, s_cbias, v_cost, sems,
):
    me = lax.axis_index("depth")
    rows, edge = lines.shape[0], moved.shape[0]
    halves = samples.shape[1]
    chunk = rows * BC
    top = bit_of(me, rounds - 1)
    small = [(order, s_order), (cgain, s_cgain), (cbias, s_cbias), (cost, v_cost)]
    pairs = list(small)
    pairs.append((bricks.at[pl.ds((1 - top) * rows, rows)], lines))
    for h in range(halves):
        span = pl.ds(h * LANES, LANES)
        pairs.append((table0, tab0.at[:, span, span]))
    pairs.append((table1, tab1))
    pairs.append((bricks.at[pl.ds(top * rows, rows)], next_lines))
    copies = [pltpu.make_async_copy(a, b, sems.at[i]) for i, (a, b) in enumerate(pairs)]
    for copy in copies:
        copy.start()

    size = BC * edge
    out_row = lax.broadcasted_iota(jnp.int32, (size, size), 0)
    in_row = lax.broadcasted_iota(jnp.int32, (size, size), 1)
    wanted = lax.rem(out_row, BC) * edge + out_row // BC
    perm[...] = jnp.where(wanted == in_row, 1.0, 0.0).astype(jnp.bfloat16)
    zero = jnp.zeros((LANES, LANES), jnp.bfloat16)
    for k in range(edge):
        for a in range(halves):
            for b in range(halves):
                if a != b:
                    tab0[k, a * LANES : (a + 1) * LANES, b * LANES : (b + 1) * LANES] = zero

    for copy in copies[: len(small)]:
        copy.wait()

    def splat(value):
        return jnp.full((SUB, LANES), value, jnp.float32)

    splats[EXT_SLOPE] = splat(egain[0] * LOG2E)
    splats[EXT_SHIFT] = splat(ebias[0] * LOG2E + math.log2(LOG2E))
    for c in range(3):
        splats[SLOPES + c] = splat(s_cgain[c] * 0.5)
        splats[SHIFTS + c] = splat(s_cbias[c] * 0.5)
    for v in range(2):
        flip = s_order[v, 0] > s_order[v, order.shape[1] - 1]
        splats[FLIPS + v] = splat(jnp.where(flip, 1.0, 0.0))
        rank = lax.bitwise_xor(me, s_order[v, 0])
        for bit in range(rounds):
            splats[FRONTS + v * rounds + bit] = splat(bit_of(rank, bit).astype(jnp.float32))

    here = lax.broadcasted_iota(jnp.int32, (chunk, chunk), 0)
    there = lax.broadcasted_iota(jnp.int32, (chunk, chunk), 1)
    low, high = v_cost[0:1, :chunk], v_cost[0:1, chunk:]
    ones = jnp.ones((chunk, LANES), jnp.bfloat16)
    for i, row in enumerate((jnp.where(top == 0, high, low), jnp.where(top == 0, low, high))):
        picked = jnp.where(here == there, row.astype(jnp.float32), 0.0).astype(jnp.bfloat16)
        levels[i] = jnp.dot(picked, ones, preferred_element_type=jnp.float32)

    copies[len(small)].wait()
    for r in range(rows):
        to_slices(lines, r, perm, moved)
    for h in range(halves):
        copies[len(small) + 1 + h].wait()
    for k in range(edge):
        resample(k, 0, moved, tab0, splats, samples)
    copies[len(small) + 1 + halves].wait()

    def step(i, carry):
        resample(i, 1, moved, tab1, splats, next_samples)
        shade_pair(i, low_bits, 0, samples, levels.at[0], splats, send, kept)
        return carry

    lax.fori_loop(0, edge, step, 0)
    copies[len(small) + 2 + halves].wait()


def second_kernel(low_bits, samples, lines, tab0, perm, levels, splats, send, kept, next_samples, moved):
    rows, edge = lines.shape[0], moved.shape[0]
    items = edge // rows

    def step(i, carry):
        to_slices(lines, i, perm, moved)
        shade_pair(i, low_bits, 1, samples, levels.at[0], splats, send, kept)
        return carry

    lax.fori_loop(0, rows, step, 0)

    def later(i, carry):
        for n in range(2):
            resample(i * 2 + n, 0, moved, tab0, splats, next_samples)
        shade_pair(rows + i, low_bits, 1, samples, levels.at[0], splats, send, kept)
        return carry

    lax.fori_loop(0, edge // 2, later, 0)


def third_kernel(low_bits, samples, moved, tab1, levels, splats, send, kept, next_samples):
    edge = samples.shape[0]

    def step(i, carry):
        resample(i, 1, moved, tab1, splats, next_samples)
        shade_pair(i, low_bits, 0, samples, levels.at[1], splats, send, kept)
        return carry

    lax.fori_loop(0, edge, step, 0)


def fourth_kernel(low_bits, samples, levels, splats, send, kept):
    edge = samples.shape[0]

    def step(i, carry):
        shade_pair(i, low_bits, 1, samples, levels.at[1], splats, send, kept)
        return carry

    lax.fori_loop(0, edge, step, 0)


VMEM = pl.BlockSpec(memory_space=pltpu.VMEM)
HBM = pl.BlockSpec(memory_space=pltpu.HBM)


def call(kernel, name, ins, outs, cycles, scratch=(), limit=4 << 20, specs=None):
    outs = tuple(jax.ShapeDtypeStruct(shape, dtype) for shape, dtype in outs)
    return pl.pallas_call(
        kernel,
        out_shape=outs,
        in_specs=specs or [VMEM] * len(ins),
        out_specs=tuple(VMEM for _ in outs),
        scratch_shapes=list(scratch),
        compiler_params=pltpu.CompilerParams(vmem_limit_bytes=limit),
        cost_estimate=pl.CostEstimate(flops=cycles * 4096, bytes_accessed=1 << 18, transcendentals=0),
        name=name,
    )(*ins)


def render(rounds, low_bits, order, cgain, cbias, egain, ebias, cost, bricks, table0, table1):
    total, edge, plane = bricks.shape
    rows = total // BC // 2
    chunk, halves, size = rows * BC, plane // LANES, BC * edge
    f32, bf16 = jnp.float32, jnp.bfloat16
    part = ((rows * halves // 2, 4, BC, LANES), f32)
    samples = ((edge, halves, chunk, LANES), f32)
    lines = ((rows, BC, edge, plane), bf16)
    moved = ((edge, chunk, plane), bf16)
    table = ((edge, plane, plane), bf16)
    square = ((size, size), bf16)
    levels = ((2, chunk, LANES), f32)
    splats = ((FRONTS + 2 * rounds, SUB, LANES), f32)
    bricks = bricks.reshape(total // BC, BC, edge, plane)
    far = lambda x: pltpu.with_memory_space_constraint(x, pltpu.HBM)
    ins = (far(order), far(cgain), far(cbias), egain, ebias, far(cost), far(bricks), far(table0), far(table1))
    specs = [HBM] * 3 + [pl.BlockSpec(memory_space=pltpu.SMEM)] * 2 + [HBM] * 4
    send0, kept0, samples1, lines_b, tab0, tab1, perm, levels_, splats_ = call(
        functools.partial(first_kernel, rounds, low_bits), "first", ins,
        (part, part, samples, lines, table, table, square, levels, splats), 6000,
        [pltpu.VMEM(*lines), pltpu.VMEM(*moved), pltpu.VMEM(*samples),
         pltpu.SMEM(order.shape, order.dtype), pltpu.SMEM(cgain.shape, f32), pltpu.SMEM(cbias.shape, f32),
         pltpu.VMEM(cost.shape, cost.dtype),
         pltpu.SemaphoreType.DMA((10 + halves,))],
        24 << 20, specs,
    )
    send1, kept1, samples_b0, moved_b = call(
        functools.partial(second_kernel, low_bits), "second", (samples1, lines_b, tab0, perm, levels_, splats_),
        (part, part, samples, moved), 3500, (), 16 << 20,
    )
    send2, kept2, samples_b1 = call(
        functools.partial(third_kernel, low_bits), "third", (samples_b0, moved_b, tab1, levels_, splats_),
        (part, part, samples), 3500, (), 16 << 20,
    )
    send3, kept3 = call(
        functools.partial(fourth_kernel, low_bits), "fourth", (samples_b1, levels_, splats_),
        (part, part), 3300, (), 8 << 20,
    )
    return splats_, [[(send0, kept0), (send1, kept1)], [(send2, kept2), (send3, kept3)]]


def merged_pair(front, kept, incoming):
    behind = 1.0 - front * incoming[3]
    ahead = 1.0 - (1.0 - front) * kept[3]
    return [kept[c] * behind + incoming[c] * ahead for c in range(4)]


def front_of(splats, v, rounds, bit):
    one = splats[FRONTS + v * rounds + bit]
    return jnp.concatenate([one] * (BC // SUB), axis=0)


def read(ref, unit):
    parts = [ref[unit, c] for c in range(4)]
    return [decode(x) for x in parts] if ref.dtype == jnp.int16 else parts


def merge_kernel(v, rounds, bit, low_bits, splats, kept, incoming, *outs):
    mine = bit_of(lax.axis_index("depth"), bit + 1)
    front = front_of(splats, v, rounds, bit)
    units = kept.shape[0]
    for i, out in enumerate(outs):
        for slot in range(units // len(outs)):
            unit = slot
            if len(outs) > 1:
                unit = spread_bit(slot, low_bits, 1 - mine if i == 0 else mine)
            done = merged_pair(front, read(kept, unit), read(incoming, unit))
            for c in range(4):
                out[slot, c] = encode(done[c]) if out.dtype == jnp.int16 else done[c]


def merge(v, rounds, bit, low_bits, split, splats, kept, incoming):
    units, tail = kept.shape[0], kept.shape[1:]
    outs = ((units, *tail), jnp.int16)
    outs = (((units // 2, *tail), jnp.int16), ((units // 2, *tail), jnp.float32)) if split else (outs,)
    kernel = functools.partial(merge_kernel, v, rounds, bit, low_bits)
    return call(kernel, "merge", (splats, kept, incoming), outs, 600)


def finish_kernel(rounds, edge, splats, *refs):
    out = refs[-1]
    units = out.shape[2] * edge // LANES
    chunks = LANES // edge
    chunk_of = lax.broadcasted_iota(jnp.int32, (SUB, LANES), 1) // edge
    for v in range(2):
        kept, near, far = refs[3 * v : 3 * v + 3]
        for unit in range(units):
            done = merged_pair(front_of(splats, v, rounds, rounds - 2), read(kept, unit), read(near, unit))
            done = merged_pair(front_of(splats, v, rounds, rounds - 1), done, read(far, unit))
            for c in range(4):
                for g in range(BC // SUB):
                    x = done[c][g * SUB : (g + 1) * SUB, :]
                    x = pltpu.roll(x, 0, 1, stride=edge, stride_axis=0)
                    for step in range(3):
                        turned = pltpu.roll(x, SUB - (1 << step), 0)
                        x = jnp.where(bit_of(chunk_of, step) == 1, turned, x)
                    x = pltpu.roll(x, 0, 1, stride=edge, stride_axis=0)
                    out[v, c, unit * chunks : (unit + 1) * chunks, g * LANES : (g + 1) * LANES] = x


def finish(rounds, edge, splats, ins):
    units = ins[0].shape[0]
    out = ((2, 4, units * LANES // edge, BC * edge), jnp.float32)
    return call(functools.partial(finish_kernel, rounds, edge), "finish", (splats, *ins), (out,), 1500)[0]


def swapped(x, bit):
    count = lax.axis_size("depth")
    return lax.ppermute(x, "depth", [(i, i ^ 1 << bit) for i in range(count)])


def shards(bricks, cost, order, color_gain, color_bias, ext_gain, ext_bias):
    bricks = bricks[0]
    total, edge, plane = bricks.shape
    count = lax.axis_size("depth")
    rounds = count.bit_length() - 1
    units = total // BC * (plane // LANES)
    low_bits = (units // count).bit_length() - 1
    table0, table1 = (jnp.asarray(t) for t in shear_tables(edge))
    splats, parts = render(
        rounds, low_bits, order, color_gain, color_bias, ext_gain, ext_bias, cost, bricks, table0, table1
    )
    last = {}
    for half in range(2):
        for v in range(2):
            send, kept = parts[half][v]
            for bit in range(rounds - 2):
                send, kept = merge(v, rounds, bit, low_bits, True, splats, kept, swapped(send, bit))
            incoming = swapped(send, rounds - 2)
            if half == 0:
                (leaving,) = merge(v, rounds, rounds - 2, low_bits, False, splats, kept, incoming)
                last[v] = swapped(leaving, rounds - 1)
            else:
                parts[half][v] = (kept, incoming)
    ins = []
    for v in range(2):
        ins += [*parts[1][v], last[v]]
    return finish(rounds, edge, splats, ins)


def solution(mesh):
    in_specs = (P("depth", "image", None, None), P("depth", "image"), P(), P(), P(), P(), P())
    out_specs = P(None, None, "depth", "image")
    return jax.shard_map(shards, mesh=mesh, in_specs=in_specs, out_specs=out_specs, check_vma=False)
```

```python
import functools
import math

import jax
import jax.numpy as jnp
import numpy as np
from jax import lax
from jax.experimental import pallas as pl
from jax.experimental.pallas import tpu as pltpu
from jax.sharding import PartitionSpec as P


BC = 16
LANES = 128
SUB = 8
SHEAR = (0.45, -0.3)
LOG2E = 1.0 / math.log(2.0)

CODE_RANGE = 32.0
CODE_STEP = 2047.0
CODE_BIAS = 32768.0


def shear_taps(brick_edge, view):
    f32 = np.float32
    slice_index = np.arange(brick_edge, dtype=f32)[:, None]
    position = np.arange(brick_edge, dtype=f32)[None, :] + f32(SHEAR[view]) * (
        slice_index - f32((brick_edge - 1) / 2.0)
    )
    anchor = np.floor(position)
    fraction = (position - anchor).astype(f32)
    low = (f32(1.0) - fraction).astype(jnp.bfloat16).astype(f32)
    high = fraction.astype(jnp.bfloat16).astype(f32)
    return anchor.astype(np.int32), low, high


def shear_lines(brick_edge, view):
    anchor, low, high = shear_taps(brick_edge, view)
    source = np.arange(brick_edge)[None, :, None]
    table = np.where(source == anchor[:, None, :], low[:, None, :], 0.0)
    return table + np.where(source == anchor[:, None, :] + 1, high[:, None, :], 0.0)


def shear_tables(edge):
    along_cols = shear_lines(edge, 0)
    along_rows = shear_lines(edge, 1)
    block = np.stack([np.kron(np.eye(LANES // edge), t) for t in along_cols])
    full = np.stack([np.kron(t, np.eye(edge)) for t in along_rows])
    lane = np.arange(LANES)
    turned = (-(lane // edge) % (LANES // edge)) * edge + lane % edge
    block = block[:, :, turned]
    full = full.reshape(edge, edge * edge, -1, LANES)[..., turned].reshape(full.shape)
    return block.astype(jnp.bfloat16), full.astype(jnp.bfloat16)


def encode(x):
    logs = jnp.log(jnp.maximum(x, 2.0**-CODE_RANGE))
    code = logs * (CODE_STEP * LOG2E) + (CODE_RANGE * CODE_STEP + 0.5)
    return (code.astype(jnp.int32) - int(CODE_BIAS)).astype(jnp.int16)


def decode(code):
    value = code.astype(jnp.int32).astype(jnp.float32)
    return jnp.exp2(value * (1.0 / CODE_STEP) + (CODE_BIAS / CODE_STEP - CODE_RANGE))


EXT_SLOPE, EXT_SHIFT, SLOPES, SHIFTS, FLIPS, FRONTS = 0, 1, 2, 5, 8, 10


def bit_of(value, bit):
    return lax.bitwise_and(lax.shift_right_logical(value, bit), 1)


def spread_bit(slot, position, bit):
    high = lax.shift_left(lax.shift_right_logical(slot, position), position + 1)
    low = lax.bitwise_and(slot, (1 << position) - 1)
    return high + low + bit * (1 << position)


def shade(item, bit, low_bits, v, samples, levels, splats, out):
    edge, halves = samples.shape[1], samples.shape[2]
    slot, group = item // 2, lax.rem(item, 2)
    unit = spread_bit(slot, low_bits, bit)
    h = lax.rem(unit, halves)
    start = pl.multiple_of((unit // halves) * BC + group * SUB, SUB)
    level = levels[pl.ds(start, SUB), :]
    flip = splats[FLIPS + v]
    ext_slope, ext_shift = splats[EXT_SLOPE], splats[EXT_SHIFT]
    shift = []
    for j in range(4):
        need = j + flip * (3 - 2 * j)
        shift.append(jnp.where(level > need, ext_shift, -1e30))
    clear = jnp.ones((SUB, LANES), jnp.float32)
    sums = [jnp.zeros((SUB, LANES), jnp.float32) for _ in range(3)]
    for k in range(edge):
        s = samples[v, k, h, pl.ds(start, SUB), :]
        passed = jnp.exp2(-jnp.exp2(s * ext_slope + shift[k // (edge // 4)]))
        beyond = clear * passed
        weight = clear - beyond
        clear = beyond
        for c in range(3):
            sums[c] = sums[c] + weight * jnp.tanh(s * splats[SLOPES + c] + splats[SHIFTS + c])
    opacity = 1.0 - clear
    place = pl.multiple_of(group * SUB, SUB)
    for c in range(3):
        out[slot, v, c, pl.ds(place, SUB), :] = (opacity + sums[c]) * 0.5
    out[slot, v, 3, pl.ds(place, SUB), :] = opacity


def to_slices(lines, r, perm, moved):
    edge = moved.shape[0]
    x = lines[r].reshape(BC * edge, lines.shape[-1])
    slices = jnp.dot(perm[...], x, preferred_element_type=jnp.float32).astype(jnp.bfloat16)
    for k in range(edge):
        place = r * BC if isinstance(r, int) else pl.multiple_of(r * BC, BC)
        moved[k, pl.ds(place, BC), :] = slices[k * BC : (k + 1) * BC, :]


def flips_of(splats):
    return [splats[FLIPS + v, 0, 0] > 0.5 for v in range(2)]


def resample(k, v, flips, moved, table, samples):
    edge, halves = samples.shape[1], samples.shape[2]
    result = jnp.dot(moved[k], table[k], preferred_element_type=jnp.float32)
    place = jnp.where(flips[v], edge - 1 - k, k)
    for h in range(halves):
        samples[v, place, h] = result[:, h * LANES : (h + 1) * LANES]


def beside(steps, items, jobs, item_fn, job_fn):
    def body(i, carry):
        for n in range(jobs // steps):
            job_fn(i * (jobs // steps) + n)
        for n in range(items // steps):
            item_fn(i * (items // steps) + n)
        return carry

    lax.fori_loop(0, steps, body, 0)


def first_kernel(
    rounds, low_bits,
    order, cgain, cbias, egain, ebias, cost, bricks, table0, table1,
    send, samples, moved_next, lines1, lines2, lines3, tab0, tab1, perm, levels, splats,
    lines0, moved, s_order, s_cgain, s_cbias, v_cost, sems,
):
    me = lax.axis_index("depth")
    rows, edge = lines0.shape[0], moved.shape[0]
    halves = samples.shape[2]
    chunk = rows * BC
    top, second = bit_of(me, rounds - 1), bit_of(me, rounds - 2)
    quarters = [
        (1 - top) * 2 + 1 - second, (1 - top) * 2 + second, top * 2 + 1 - second, top * 2 + second
    ]
    small = [(order, s_order), (cgain, s_cgain), (cbias, s_cbias), (cost, v_cost)]
    pairs = list(small)
    pairs.append((bricks.at[pl.ds(quarters[0] * rows, rows)], lines0))
    for h in range(halves):
        span = pl.ds(h * LANES, LANES)
        pairs.append((table0, tab0.at[:, span, span]))
    pairs.append((table1, tab1))
    for quarter, lines in zip(quarters[1:], (lines1, lines2, lines3)):
        pairs.append((bricks.at[pl.ds(quarter * rows, rows)], lines))
    copies = [pltpu.make_async_copy(a, b, sems.at[i]) for i, (a, b) in enumerate(pairs)]
    for copy in copies:
        copy.start()

    size = BC * edge
    out_row = lax.broadcasted_iota(jnp.int32, (size, size), 0)
    in_row = lax.broadcasted_iota(jnp.int32, (size, size), 1)
    wanted = lax.rem(out_row, BC) * edge + out_row // BC
    perm[...] = jnp.where(wanted == in_row, 1.0, 0.0).astype(jnp.bfloat16)
    zero = jnp.zeros((LANES, LANES), jnp.bfloat16)
    for k in range(edge):
        for a in range(halves):
            for b in range(halves):
                if a != b:
                    tab0[k, a * LANES : (a + 1) * LANES, b * LANES : (b + 1) * LANES] = zero

    for copy in copies[: len(small)]:
        copy.wait()

    def splat(value):
        return jnp.full((SUB, LANES), value, jnp.float32)

    splats[EXT_SLOPE] = splat(egain[0] * LOG2E)
    splats[EXT_SHIFT] = splat(ebias[0] * LOG2E + math.log2(LOG2E))
    for c in range(3):
        splats[SLOPES + c] = splat(s_cgain[c] * 0.5)
        splats[SHIFTS + c] = splat(s_cbias[c] * 0.5)
    flips = []
    for v in range(2):
        flips.append(s_order[v, 0] > s_order[v, order.shape[1] - 1])
        splats[FLIPS + v] = splat(jnp.where(flips[v], 1.0, 0.0))
        rank = lax.bitwise_xor(me, s_order[v, 0])
        for bit in range(rounds):
            splats[FRONTS + v * rounds + bit] = splat(bit_of(rank, bit).astype(jnp.float32))

    total = v_cost.shape[1]
    here = lax.broadcasted_iota(jnp.int32, (chunk, total), 0)
    there = lax.broadcasted_iota(jnp.int32, (chunk, total), 1)
    row = v_cost[...].astype(jnp.float32)
    ones = jnp.ones((total, LANES), jnp.bfloat16)
    for i, quarter in enumerate(quarters):
        picked = jnp.where(here + quarter * chunk == there, row, 0.0).astype(jnp.bfloat16)
        levels[i] = jnp.dot(picked, ones, preferred_element_type=jnp.float32)

    copies[len(small)].wait()
    for r in range(rows):
        to_slices(lines0, r, perm, moved)
    for h in range(halves):
        copies[len(small) + 1 + h].wait()
    for k in range(edge):
        resample(k, 0, flips, moved, tab0, samples)
    for copy in copies[len(small) + 1 + halves :]:
        copy.wait()

    mine = bit_of(me, 0)

    def item(v):
        return lambda i: shade(i, 1 - mine, low_bits, v, samples, levels.at[0], splats, send)

    count = chunk // SUB * halves // 2
    beside(2, count, edge, item(0), lambda k: resample(k, 1, flips, moved, tab1, samples))
    beside(2, count, rows, item(1), lambda r: to_slices(lines1, r, perm, moved_next))


def second_kernel(low_bits, samples, moved_next, tab0, tab1, levels, splats, kept, samples_next):
    mine = bit_of(lax.axis_index("depth"), 0)
    edge = samples.shape[1]
    count = samples.shape[3] // SUB * samples.shape[2] // 2
    flips = flips_of(splats)
    for v, table in enumerate((tab0, tab1)):
        beside(
            2, count, edge,
            lambda i: shade(i, mine, low_bits, v, samples, levels.at[0], splats, kept),
            lambda k: resample(k, v, flips, moved_next, table, samples_next),
        )


def quarter_kernel(low_bits, index, last, *refs):
    if last:
        samples, levels, splats, send, kept = refs
    else:
        samples, lines, tab0, tab1, perm, levels, splats, send, kept, samples_next, moved = refs
    mine = bit_of(lax.axis_index("depth"), 0)
    edge = samples.shape[1]
    count = samples.shape[3] // SUB * samples.shape[2] // 2
    flips = flips_of(splats)

    def items(v):
        def both(i):
            shade(i, 1 - mine, low_bits, v, samples, levels.at[index], splats, send)
            shade(i, mine, low_bits, v, samples, levels.at[index], splats, kept)

        return both

    def jobs(k):
        resample(k, 0, flips, moved, tab0, samples_next)
        resample(k, 1, flips, moved, tab1, samples_next)

    if last:
        beside(4, count, 0, items(0), None)
        beside(4, count, 0, items(1), None)
    else:
        rows = lines.shape[0]
        beside(4, count, rows, items(0), lambda r: to_slices(lines, r, perm, moved))
        beside(4, count, edge, items(1), jobs)


VMEM = pl.BlockSpec(memory_space=pltpu.VMEM)
HBM = pl.BlockSpec(memory_space=pltpu.HBM)


def call(kernel, ins, outs, cycles, scratch=(), limit=4 << 20, specs=None):
    outs = tuple(jax.ShapeDtypeStruct(shape, dtype) for shape, dtype in outs)
    return pl.pallas_call(
        kernel,
        out_shape=outs,
        in_specs=specs or [VMEM] * len(ins),
        out_specs=tuple(VMEM for _ in outs),
        scratch_shapes=list(scratch),
        compiler_params=pltpu.CompilerParams(vmem_limit_bytes=limit),
        cost_estimate=pl.CostEstimate(flops=cycles * 4096, bytes_accessed=1 << 18, transcendentals=0),
    )(*ins)


def render(rounds, low_bits, order, cgain, cbias, egain, ebias, cost, bricks, table0, table1):
    total, edge, plane = bricks.shape
    rows = total // BC // 4
    chunk, halves, size = rows * BC, plane // LANES, BC * edge
    f32, bf16 = jnp.float32, jnp.bfloat16
    part = ((rows * halves // 2, 2, 4, BC, LANES), f32)
    samples = ((2, edge, halves, chunk, LANES), f32)
    lines = ((rows, BC, edge, plane), bf16)
    moved = ((edge, chunk, plane), bf16)
    table = ((edge, plane, plane), bf16)
    square = ((size, size), bf16)
    levels = ((4, chunk, LANES), f32)
    splats = ((FRONTS + 2 * rounds, SUB, LANES), f32)
    bricks = bricks.reshape(total // BC, BC, edge, plane)
    far = lambda x: pltpu.with_memory_space_constraint(x, pltpu.HBM)
    ins = (far(order), far(cgain), far(cbias), egain, ebias, far(cost), far(bricks), far(table0), far(table1))
    specs = [HBM] * 3 + [pl.BlockSpec(memory_space=pltpu.SMEM)] * 2 + [HBM] * 4
    send0, samples0, moved1, _, lines2, lines3, tab0, tab1, perm, levels_, splats_ = call(
        functools.partial(first_kernel, rounds, low_bits), ins,
        (part, samples, moved, lines, lines, lines, table, table, square, levels, splats), 4000,
        [pltpu.VMEM(*lines), pltpu.VMEM(*moved),
         pltpu.SMEM(order.shape, order.dtype), pltpu.SMEM(cgain.shape, f32), pltpu.SMEM(cbias.shape, f32),
         pltpu.VMEM(cost.shape, cost.dtype), pltpu.SemaphoreType.DMA((9 + halves,))],
        20 << 20, specs,
    )
    kept0, samples1 = call(
        functools.partial(second_kernel, low_bits),
        (samples0, moved1, tab0, tab1, levels_, splats_), (part, samples), 1800, (), 14 << 20,
    )
    send1, kept1, samples2, _ = call(
        functools.partial(quarter_kernel, low_bits, 1, False),
        (samples1, lines2, tab0, tab1, perm, levels_, splats_), (part, part, samples, moved), 3500, (), 14 << 20,
    )
    send2, kept2, samples3, _ = call(
        functools.partial(quarter_kernel, low_bits, 2, False),
        (samples2, lines3, tab0, tab1, perm, levels_, splats_), (part, part, samples, moved), 3500, (), 14 << 20,
    )
    send3, kept3 = call(
        functools.partial(quarter_kernel, low_bits, 3, True),
        (samples3, levels_, splats_), (part, part), 3300, (), 8 << 20,
    )
    return splats_, [(send0, kept0), (send1, kept1), (send2, kept2), (send3, kept3)]


def merged_pair(front, kept, incoming):
    behind = 1.0 - front * incoming[3]
    ahead = 1.0 - (1.0 - front) * kept[3]
    return [kept[c] * behind + incoming[c] * ahead for c in range(4)]


def front_of(splats, v, rounds, bit):
    one = splats[FRONTS + v * rounds + bit]
    return jnp.concatenate([one] * (BC // SUB), axis=0)


def read(ref, unit, v):
    parts = [ref[unit, v, c] for c in range(4)]
    return [decode(x) for x in parts] if ref.dtype == jnp.int16 else parts


def merge_kernel(rounds, bit, many, low_bits, splats, kept, *refs):
    incoming, outs = refs[:many], refs[many:]
    mine = bit_of(lax.axis_index("depth"), bit + many)
    units = kept.shape[0]
    for v in range(2):
        for i, out in enumerate(outs):
            for slot in range(units // len(outs)):
                unit = slot
                if len(outs) > 1:
                    unit = spread_bit(slot, low_bits, 1 - mine if i == 0 else mine)
                done = read(kept, unit, v)
                for n, came in enumerate(incoming):
                    done = merged_pair(front_of(splats, v, rounds, bit + n), done, read(came, unit, v))
                for c in range(4):
                    out[slot, v, c] = encode(done[c]) if out.dtype == jnp.int16 else done[c]


def merge(rounds, bit, low_bits, types, splats, kept, incoming):
    units, tail = kept.shape[0], kept.shape[1:]
    outs = tuple(((units // len(types), *tail), t) for t in types)
    kernel = functools.partial(merge_kernel, rounds, bit, len(incoming), low_bits)
    return call(kernel, (splats, kept, *incoming), outs, 300)


def finish_kernel(rounds, bit, edge, splats, kept, *refs):
    incoming, out = refs[:-1], refs[-1]
    chunks = LANES // edge
    chunk_of = lax.broadcasted_iota(jnp.int32, (SUB, LANES), 1) // edge
    for v in range(2):
        for unit in range(kept.shape[0]):
            done = read(kept, unit, v)
            for n, came in enumerate(incoming):
                done = merged_pair(front_of(splats, v, rounds, bit + n), done, read(came, unit, v))
            for c in range(4):
                for g in range(BC // SUB):
                    x = done[c][g * SUB : (g + 1) * SUB, :]
                    x = pltpu.roll(x, 0, 1, stride=edge, stride_axis=0)
                    for step in range(3):
                        turned = pltpu.roll(x, SUB - (1 << step), 0)
                        x = jnp.where(bit_of(chunk_of, step) == 1, turned, x)
                    x = pltpu.roll(x, 0, 1, stride=edge, stride_axis=0)
                    out[v, c, unit * chunks : (unit + 1) * chunks, g * LANES : (g + 1) * LANES] = x


def finish(rounds, bit, edge, splats, kept, incoming):
    units = kept.shape[0]
    out = ((2, 4, units * LANES // edge, BC * edge), jnp.float32)
    return call(functools.partial(finish_kernel, rounds, bit, edge), (splats, kept, *incoming), (out,), 1500)[0]


def swapped(x, bit):
    count = lax.axis_size("depth")
    return lax.ppermute(x, "depth", [(i, i ^ 1 << bit) for i in range(count)])


def shards(bricks, cost, order, color_gain, color_bias, ext_gain, ext_bias):
    bricks = bricks[0]
    total, edge, plane = bricks.shape
    count = lax.axis_size("depth")
    rounds = count.bit_length() - 1
    units = total // BC * (plane // LANES)
    low_bits = (units // count).bit_length() - 1
    table0, table1 = (jnp.asarray(t) for t in shear_tables(edge))
    splats, parts = render(
        rounds, low_bits, order, color_gain, color_bias, ext_gain, ext_bias, cost, bricks, table0, table1
    )
    f32, i16 = jnp.float32, jnp.int16
    near = rounds - 2

    def close(index):
        send, kept = parts[index]
        for bit in range(near - 1):
            incoming = swapped(send, bit)
            send, kept = merge(rounds, bit, low_bits, (f32, f32), splats, kept, [incoming])
        return kept, swapped(send, near - 1)

    def leave(index):
        kept, incoming = close(index)
        (done,) = merge(rounds, near - 1, low_bits, (i16,), splats, kept, [incoming])
        return swapped(done, near)

    across = leave(0)
    kept, incoming = close(1)
    (done,) = merge(rounds, near - 1, low_bits, (i16,), splats, kept, [incoming, across])
    top = swapped(done, near + 1)
    across = leave(2)
    kept, incoming = close(3)
    return finish(rounds, near - 1, edge, splats, kept, [incoming, across, top])


def solution(mesh):
    in_specs = (P("depth", "image", None, None), P("depth", "image"), P(), P(), P(), P(), P())
    out_specs = P(None, None, "depth", "image")

    return jax.shard_map(shards, mesh=mesh, in_specs=in_specs, out_specs=out_specs, check_vma=False)
```

```python
import functools
import math

import jax
import jax.numpy as jnp
import numpy as np
from jax import lax
from jax.experimental import pallas as pl
from jax.experimental.pallas import tpu as pltpu
from jax.sharding import PartitionSpec as P


BC = 16
LANES = 128
SUB = 8
SHEAR = (0.45, -0.3)
LOG2E = 1.0 / math.log(2.0)

CODE_RANGE = 32.0
CODE_STEP = 2047.0
CODE_BIAS = 32768.0


def shear_taps(brick_edge, view):
    f32 = np.float32
    slice_index = np.arange(brick_edge, dtype=f32)[:, None]
    position = np.arange(brick_edge, dtype=f32)[None, :] + f32(SHEAR[view]) * (
        slice_index - f32((brick_edge - 1) / 2.0)
    )
    anchor = np.floor(position)
    fraction = (position - anchor).astype(f32)
    low = (f32(1.0) - fraction).astype(jnp.bfloat16).astype(f32)
    high = fraction.astype(jnp.bfloat16).astype(f32)
    return anchor.astype(np.int32), low, high


def shear_lines(brick_edge, view):
    anchor, low, high = shear_taps(brick_edge, view)
    source = np.arange(brick_edge)[None, :, None]
    table = np.where(source == anchor[:, None, :], low[:, None, :], 0.0)
    return table + np.where(source == anchor[:, None, :] + 1, high[:, None, :], 0.0)


def shear_weights(edge):
    lane = np.arange(LANES)
    turned = (-(lane // edge) % (LANES // edge)) * edge + lane % edge
    cols = np.tile(shear_lines(edge, 0), (1, 1, LANES // edge))
    rows = np.repeat(shear_lines(edge, 1), edge, axis=2)
    rows = rows.reshape(edge, edge, -1, LANES)[..., turned].transpose(0, 2, 1, 3)
    return cols.astype(np.float32), rows.astype(np.float32)


def encode(x):
    logs = jnp.log(jnp.maximum(x, 2.0**-CODE_RANGE))
    code = logs * (CODE_STEP * LOG2E) + (CODE_RANGE * CODE_STEP + 0.5)
    return (code.astype(jnp.int32) - int(CODE_BIAS)).astype(jnp.int16)


def decode(code):
    value = code.astype(jnp.int32).astype(jnp.float32)
    return jnp.exp2(value * (1.0 / CODE_STEP) + (CODE_BIAS / CODE_STEP - CODE_RANGE))


EXT_SLOPE, EXT_SHIFT, SLOPES, SHIFTS, FLIPS, FRONTS = 0, 1, 2, 5, 8, 10


def bit_of(value, bit):
    return lax.bitwise_and(lax.shift_right_logical(value, bit), 1)


def spread_bit(slot, position, bit):
    high = lax.shift_left(lax.shift_right_logical(slot, position), position + 1)
    low = lax.bitwise_and(slot, (1 << position) - 1)
    return high + low + bit * (1 << position)


def shade(item, bit, low_bits, v, samples, levels, splats, out):
    edge, halves = samples.shape[1], samples.shape[2]
    slot, group = item // 2, lax.rem(item, 2)
    unit = spread_bit(slot, low_bits, bit)
    h = lax.rem(unit, halves)
    start = pl.multiple_of((unit // halves) * BC + group * SUB, SUB)
    level = levels[pl.ds(start, SUB), :]
    flip = splats[FLIPS + v]
    ext_slope, ext_shift = splats[EXT_SLOPE], splats[EXT_SHIFT]
    shift = []
    for j in range(4):
        need = j + flip * (3 - 2 * j)
        shift.append(jnp.where(level > need, ext_shift, -1e30))
    clear = jnp.ones((SUB, LANES), jnp.float32)
    sums = [jnp.zeros((SUB, LANES), jnp.float32) for _ in range(3)]
    for k in range(edge):
        s = samples[v, k, h, pl.ds(start, SUB), :]
        passed = jnp.exp2(-jnp.exp2(s * ext_slope + shift[k // (edge // 4)]))
        beyond = clear * passed
        weight = clear - beyond
        clear = beyond
        for c in range(3):
            sums[c] = sums[c] + weight * jnp.tanh(s * splats[SLOPES + c] + splats[SHIFTS + c])
    opacity = 1.0 - clear
    place = pl.multiple_of(group * SUB, SUB)
    for c in range(3):
        out[slot, v, c, pl.ds(place, SUB), :] = (opacity + sums[c]) * 0.5
    out[slot, v, 3, pl.ds(place, SUB), :] = opacity


def wide(ref, *index):
    return jnp.concatenate([ref[(*index, h)] for h in range(ref.shape[len(index)])], axis=-1)


def to_slices(lines, r, perm, moved):
    edge, halves = moved.shape[0], moved.shape[1]
    x = jnp.concatenate([lines[r, h].reshape(BC * edge, LANES) for h in range(halves)], axis=-1)
    slices = jnp.dot(wide(perm), x, preferred_element_type=jnp.float32).astype(jnp.bfloat16)
    place = r * BC if isinstance(r, int) else pl.multiple_of(r * BC, BC)
    for k in range(edge):
        for h in range(halves):
            moved[k, h, pl.ds(place, BC), :] = slices[k * BC : (k + 1) * BC, h * LANES : (h + 1) * LANES]


def flips_of(splats):
    return [splats[FLIPS + v, 0, 0] > 0.5 for v in range(2)]


def resample(k, v, flips, moved, table, samples):
    edge, halves = samples.shape[1], samples.shape[2]
    result = jnp.dot(wide(moved, k), wide(table, k), preferred_element_type=jnp.float32)
    place = jnp.where(flips[v], edge - 1 - k, k)
    for h in range(halves):
        samples[v, place, h] = result[:, h * LANES : (h + 1) * LANES]


def beside(steps, items, jobs, item_fn, job_fn):
    def body(i, carry):
        for n in range(jobs // steps):
            job_fn(i * (jobs // steps) + n)
        for n in range(items // steps):
            item_fn(i * (items // steps) + n)
        return carry

    lax.fori_loop(0, steps, body, 0)


def first_kernel(
    rounds, low_bits,
    order, cgain, cbias, egain, ebias, cost, bricks, weights0, weights1,
    send, samples, moved_next, lines1, lines2, lines3, tab0, tab1, perm, levels, splats,
    lines0, moved, w0, w1, s_order, s_cgain, s_cbias, v_cost, sems,
):
    me = lax.axis_index("depth")
    rows, edge = lines0.shape[0], moved.shape[0]
    halves = samples.shape[2]
    chunk = rows * BC
    top, second = bit_of(me, rounds - 1), bit_of(me, rounds - 2)
    quarters = [
        (1 - top) * 2 + 1 - second, (1 - top) * 2 + second, top * 2 + 1 - second, top * 2 + second
    ]
    small = [(weights0, w0), (weights1, w1), (order, s_order), (cgain, s_cgain), (cbias, s_cbias), (cost, v_cost)]
    pairs = list(small)
    for quarter, lines in zip(quarters, (lines0, lines1, lines2, lines3)):
        for h in range(halves):
            span = pl.ds(h * LANES, LANES)
            pairs.append((bricks.at[pl.ds(quarter * rows, rows), :, :, span], lines.at[:, h]))
    copies = [pltpu.make_async_copy(a, b, sems.at[i]) for i, (a, b) in enumerate(pairs)]
    for copy in copies:
        copy.start()
    ready = [copies[len(small) + q * halves : len(small) + (q + 1) * halves] for q in range(4)]

    size = BC * edge
    for h in range(halves):
        out_row = lax.broadcasted_iota(jnp.int32, (size, LANES), 0)
        in_row = lax.broadcasted_iota(jnp.int32, (size, LANES), 1) + h * LANES
        wanted = lax.rem(out_row, BC) * edge + out_row // BC
        perm[h] = jnp.where(wanted == in_row, 1.0, 0.0).astype(jnp.bfloat16)

    for copy in copies[: len(small)]:
        copy.wait()

    def splat(value):
        return jnp.full((SUB, LANES), value, jnp.float32)

    splats[EXT_SLOPE] = splat(egain[0] * LOG2E)
    splats[EXT_SHIFT] = splat(ebias[0] * LOG2E + math.log2(LOG2E))
    for c in range(3):
        splats[SLOPES + c] = splat(s_cgain[c] * 0.5)
        splats[SHIFTS + c] = splat(s_cbias[c] * 0.5)
    flips = []
    for v in range(2):
        flips.append(s_order[v, 0] > s_order[v, order.shape[1] - 1])
        splats[FLIPS + v] = splat(jnp.where(flips[v], 1.0, 0.0))
        rank = lax.bitwise_xor(me, s_order[v, 0])
        for bit in range(rounds):
            splats[FRONTS + v * rounds + bit] = splat(bit_of(rank, bit).astype(jnp.float32))

    total = v_cost.shape[1]
    here = lax.broadcasted_iota(jnp.int32, (chunk, total), 0)
    there = lax.broadcasted_iota(jnp.int32, (chunk, total), 1)
    row = v_cost[...].astype(jnp.float32)
    ones = jnp.ones((total, LANES), jnp.bfloat16)
    for i, quarter in enumerate(quarters):
        picked = jnp.where(here + quarter * chunk == there, row, 0.0).astype(jnp.bfloat16)
        levels[i] = jnp.dot(picked, ones, preferred_element_type=jnp.float32)

    tile = LANES // edge
    lane = lax.broadcasted_iota(jnp.int32, (edge, LANES), 1)
    source = lax.broadcasted_iota(jnp.int32, (edge, LANES), 0)
    masks = [jnp.where(lane // edge == (-y) % tile, 1.0, 0.0) for y in range(tile)]
    column = jnp.where(lax.rem(lane, edge) == source, 1.0, 0.0)
    blank = jnp.zeros((edge, LANES), jnp.bfloat16)

    def build(k, carry):
        cols = w0[k]
        blocks = [(cols * masks[y]).astype(jnp.bfloat16) for y in range(tile)]
        for y in range(edge):
            for h in range(halves):
                span = pl.ds(y * edge, edge)
                tab0[k, h, span, :] = blocks[y % tile] if y // tile == h else blank
                tab1[k, h, span, :] = (column * w1[k, h, y : y + 1, :]).astype(jnp.bfloat16)
        return carry

    lax.fori_loop(0, edge, build, 0)

    for copy in ready[0]:
        copy.wait()
    for r in range(rows):
        to_slices(lines0, r, perm, moved)
    for k in range(edge):
        resample(k, 0, flips, moved, tab0, samples)

    mine = bit_of(me, 0)

    def item(v):
        return lambda i: shade(i, 1 - mine, low_bits, v, samples, levels.at[0], splats, send)

    count = chunk // SUB * halves // 2
    beside(2, count, edge, item(0), lambda k: resample(k, 1, flips, moved, tab1, samples))
    for copy in ready[1]:
        copy.wait()
    beside(2, count, rows, item(1), lambda r: to_slices(lines1, r, perm, moved_next))
    for copy in ready[2] + ready[3]:
        copy.wait()


def second_kernel(low_bits, samples, moved_next, tab0, tab1, levels, splats, kept, samples_next):
    mine = bit_of(lax.axis_index("depth"), 0)
    edge = samples.shape[1]
    count = samples.shape[3] // SUB * samples.shape[2] // 2
    flips = flips_of(splats)
    for v, table in enumerate((tab0, tab1)):
        beside(
            2, count, edge,
            lambda i: shade(i, mine, low_bits, v, samples, levels.at[0], splats, kept),
            lambda k: resample(k, v, flips, moved_next, table, samples_next),
        )


def quarter_kernel(low_bits, index, last, *refs):
    if last:
        samples, levels, splats, send, kept = refs
    else:
        samples, lines, tab0, tab1, perm, levels, splats, send, kept, samples_next, moved = refs
    mine = bit_of(lax.axis_index("depth"), 0)
    edge = samples.shape[1]
    count = samples.shape[3] // SUB * samples.shape[2] // 2
    flips = flips_of(splats)

    def items(v):
        def both(i):
            shade(i, 1 - mine, low_bits, v, samples, levels.at[index], splats, send)
            shade(i, mine, low_bits, v, samples, levels.at[index], splats, kept)

        return both

    def jobs(k):
        resample(k, 0, flips, moved, tab0, samples_next)
        resample(k, 1, flips, moved, tab1, samples_next)

    if last:
        beside(4, count, 0, items(0), None)
        beside(4, count, 0, items(1), None)
    else:
        rows = lines.shape[0]
        beside(4, count, rows, items(0), lambda r: to_slices(lines, r, perm, moved))
        beside(4, count, edge, items(1), jobs)


VMEM = pl.BlockSpec(memory_space=pltpu.VMEM)
HBM = pl.BlockSpec(memory_space=pltpu.HBM)


def call(kernel, ins, outs, cycles, scratch=(), limit=4 << 20, specs=None):
    outs = tuple(jax.ShapeDtypeStruct(shape, dtype) for shape, dtype in outs)
    return pl.pallas_call(
        kernel,
        out_shape=outs,
        in_specs=specs or [VMEM] * len(ins),
        out_specs=tuple(VMEM for _ in outs),
        scratch_shapes=list(scratch),
        compiler_params=pltpu.CompilerParams(vmem_limit_bytes=limit),
        cost_estimate=pl.CostEstimate(flops=cycles * 4096, bytes_accessed=1 << 18, transcendentals=0),
    )(*ins)


def render(rounds, low_bits, order, cgain, cbias, egain, ebias, cost, bricks, weights0, weights1):
    total, edge, plane = bricks.shape
    rows = total // BC // 4
    chunk, halves, size = rows * BC, plane // LANES, BC * edge
    f32, bf16 = jnp.float32, jnp.bfloat16
    part = ((rows * halves // 2, 2, 4, BC, LANES), f32)
    samples = ((2, edge, halves, chunk, LANES), f32)
    lines = ((rows, halves, BC, edge, LANES), bf16)
    moved = ((edge, halves, chunk, LANES), bf16)
    table = ((edge, halves, plane, LANES), bf16)
    square = ((size // LANES, size, LANES), bf16)
    levels = ((4, chunk, LANES), f32)
    splats = ((FRONTS + 2 * rounds, SUB, LANES), f32)
    bricks = bricks.reshape(total // BC, BC, edge, plane)
    far = lambda x: pltpu.with_memory_space_constraint(x, pltpu.HBM)
    ins = (far(order), far(cgain), far(cbias), egain, ebias, far(cost), far(bricks), far(weights0), far(weights1))
    specs = [HBM] * 3 + [pl.BlockSpec(memory_space=pltpu.SMEM)] * 2 + [HBM] * 4
    send0, samples0, moved1, _, lines2, lines3, tab0, tab1, perm, levels_, splats_ = call(
        functools.partial(first_kernel, rounds, low_bits), ins,
        (part, samples, moved, lines, lines, lines, table, table, square, levels, splats), 4000,
        [pltpu.VMEM(*lines), pltpu.VMEM(*moved), pltpu.VMEM(weights0.shape, f32), pltpu.VMEM(weights1.shape, f32),
         pltpu.SMEM(order.shape, order.dtype), pltpu.SMEM(cgain.shape, f32), pltpu.SMEM(cbias.shape, f32),
         pltpu.VMEM(cost.shape, cost.dtype), pltpu.SemaphoreType.DMA((6 + 4 * halves,))],
        20 << 20, specs,
    )
    kept0, samples1 = call(
        functools.partial(second_kernel, low_bits),
        (samples0, moved1, tab0, tab1, levels_, splats_), (part, samples), 1800, (), 14 << 20,
    )
    send1, kept1, samples2, _ = call(
        functools.partial(quarter_kernel, low_bits, 1, False),
        (samples1, lines2, tab0, tab1, perm, levels_, splats_), (part, part, samples, moved), 3500, (), 14 << 20,
    )
    send2, kept2, samples3, _ = call(
        functools.partial(quarter_kernel, low_bits, 2, False),
        (samples2, lines3, tab0, tab1, perm, levels_, splats_), (part, part, samples, moved), 3500, (), 14 << 20,
    )
    send3, kept3 = call(
        functools.partial(quarter_kernel, low_bits, 3, True),
        (samples3, levels_, splats_), (part, part), 3300, (), 8 << 20,
    )
    return splats_, [(send0, kept0), (send1, kept1), (send2, kept2), (send3, kept3)]


def merged_pair(front, kept, incoming):
    behind = 1.0 - front * incoming[3]
    ahead = 1.0 - (1.0 - front) * kept[3]
    return [kept[c] * behind + incoming[c] * ahead for c in range(4)]


def front_of(splats, v, rounds, bit):
    one = splats[FRONTS + v * rounds + bit]
    return jnp.concatenate([one] * (BC // SUB), axis=0)


def read(ref, unit, v):
    parts = [ref[unit, v, c] for c in range(4)]
    return [decode(x) for x in parts] if ref.dtype == jnp.int16 else parts


def merge_kernel(rounds, bit, many, low_bits, splats, kept, *refs):
    incoming, outs = refs[:many], refs[many:]
    mine = bit_of(lax.axis_index("depth"), bit + many)
    units = kept.shape[0]
    for v in range(2):
        for i, out in enumerate(outs):
            for slot in range(units // len(outs)):
                unit = slot
                if len(outs) > 1:
                    unit = spread_bit(slot, low_bits, 1 - mine if i == 0 else mine)
                done = read(kept, unit, v)
                for n, came in enumerate(incoming):
                    done = merged_pair(front_of(splats, v, rounds, bit + n), done, read(came, unit, v))
                for c in range(4):
                    out[slot, v, c] = encode(done[c]) if out.dtype == jnp.int16 else done[c]


def merge(rounds, bit, low_bits, types, splats, kept, incoming):
    units, tail = kept.shape[0], kept.shape[1:]
    outs = tuple(((units // len(types), *tail), t) for t in types)
    kernel = functools.partial(merge_kernel, rounds, bit, len(incoming), low_bits)
    return call(kernel, (splats, kept, *incoming), outs, 300)


def finish_kernel(rounds, bit, edge, splats, kept, *refs):
    incoming, out = refs[:-1], refs[-1]
    chunks = LANES // edge
    chunk_of = lax.broadcasted_iota(jnp.int32, (SUB, LANES), 1) // edge
    for v in range(2):
        for unit in range(kept.shape[0]):
            done = read(kept, unit, v)
            for n, came in enumerate(incoming):
                done = merged_pair(front_of(splats, v, rounds, bit + n), done, read(came, unit, v))
            for c in range(4):
                for g in range(BC // SUB):
                    x = done[c][g * SUB : (g + 1) * SUB, :]
                    x = pltpu.roll(x, 0, 1, stride=edge, stride_axis=0)
                    for step in range(3):
                        turned = pltpu.roll(x, SUB - (1 << step), 0)
                        x = jnp.where(bit_of(chunk_of, step) == 1, turned, x)
                    x = pltpu.roll(x, 0, 1, stride=edge, stride_axis=0)
                    out[v, c, unit * chunks : (unit + 1) * chunks, g * LANES : (g + 1) * LANES] = x


def finish(rounds, bit, edge, splats, kept, incoming):
    units = kept.shape[0]
    out = ((2, 4, units * LANES // edge, BC * edge), jnp.float32)
    return call(functools.partial(finish_kernel, rounds, bit, edge), (splats, kept, *incoming), (out,), 1500)[0]


def swapped(x, bit):
    count = lax.axis_size("depth")
    return lax.ppermute(x, "depth", [(i, i ^ 1 << bit) for i in range(count)])


def shards(bricks, cost, order, color_gain, color_bias, ext_gain, ext_bias):
    bricks = bricks[0]
    total, edge, plane = bricks.shape
    count = lax.axis_size("depth")
    rounds = count.bit_length() - 1
    units = total // BC * (plane // LANES)
    low_bits = (units // count).bit_length() - 1
    weights0, weights1 = (jnp.asarray(t) for t in shear_weights(edge))
    splats, parts = render(
        rounds, low_bits, order, color_gain, color_bias, ext_gain, ext_bias, cost, bricks, weights0, weights1
    )
    f32, i16 = jnp.float32, jnp.int16
    near = rounds - 2

    def close(index):
        send, kept = parts[index]
        for bit in range(near - 1):
            incoming = swapped(send, bit)
            send, kept = merge(rounds, bit, low_bits, (f32, f32), splats, kept, [incoming])
        return kept, swapped(send, near - 1)

    def leave(index):
        kept, incoming = close(index)
        (done,) = merge(rounds, near - 1, low_bits, (i16,), splats, kept, [incoming])
        return swapped(done, near)

    across = leave(0)
    kept, incoming = close(1)
    (done,) = merge(rounds, near - 1, low_bits, (i16,), splats, kept, [incoming, across])
    top = swapped(done, near + 1)
    across = leave(2)
    kept, incoming = close(3)
    return finish(rounds, near - 1, edge, splats, kept, [incoming, across, top])


def solution(mesh):
    in_specs = (P("depth", "image", None, None), P("depth", "image"), P(), P(), P(), P(), P())
    out_specs = P(None, None, "depth", "image")

    return jax.shard_map(shards, mesh=mesh, in_specs=in_specs, out_specs=out_specs, check_vma=False)
```

```python
import functools
import math

import jax
import jax.numpy as jnp
import numpy as np
from jax import lax
from jax.experimental import pallas as pl
from jax.experimental.pallas import tpu as pltpu
from jax.sharding import PartitionSpec as P


BC = 16
LANES = 128
SUB = 8
SHEAR = (0.45, -0.3)
LOG2E = 1.0 / math.log(2.0)

CODE_RANGE = 32.0
CODE_STEP = 2047.0
CODE_BIAS = 32768.0


def shear_taps(brick_edge, view):
    f32 = np.float32
    slice_index = np.arange(brick_edge, dtype=f32)[:, None]
    position = np.arange(brick_edge, dtype=f32)[None, :] + f32(SHEAR[view]) * (
        slice_index - f32((brick_edge - 1) / 2.0)
    )
    anchor = np.floor(position)
    fraction = (position - anchor).astype(f32)
    low = (f32(1.0) - fraction).astype(jnp.bfloat16).astype(f32)
    high = fraction.astype(jnp.bfloat16).astype(f32)
    return anchor.astype(np.int32), low, high


def shear_lines(brick_edge, view):
    anchor, low, high = shear_taps(brick_edge, view)
    source = np.arange(brick_edge)[None, :, None]
    table = np.where(source == anchor[:, None, :], low[:, None, :], 0.0)
    return table + np.where(source == anchor[:, None, :] + 1, high[:, None, :], 0.0)


def shear_weights(edge):
    lane = np.arange(LANES)
    turned = (-(lane // edge) % (LANES // edge)) * edge + lane % edge
    cols = np.tile(shear_lines(edge, 0), (1, 1, LANES // edge))
    rows = np.repeat(shear_lines(edge, 1), edge, axis=2)
    rows = rows.reshape(edge, edge, -1, LANES)[..., turned].transpose(0, 2, 1, 3)
    return cols.astype(np.float32), rows.astype(np.float32)


def encode(x):
    logs = jnp.log(jnp.maximum(x, 2.0**-CODE_RANGE))
    code = logs * (CODE_STEP * LOG2E) + (CODE_RANGE * CODE_STEP + 0.5)
    return (code.astype(jnp.int32) - int(CODE_BIAS)).astype(jnp.int16)


def decode(code):
    value = code.astype(jnp.int32).astype(jnp.float32)
    return jnp.exp2(value * (1.0 / CODE_STEP) + (CODE_BIAS / CODE_STEP - CODE_RANGE))


EXT_SLOPE, EXT_SHIFT, SLOPES, SHIFTS, FLIPS, FRONTS = 0, 1, 2, 5, 8, 10


def bit_of(value, bit):
    return lax.bitwise_and(lax.shift_right_logical(value, bit), 1)


def spread_bit(slot, position, bit):
    high = lax.shift_left(lax.shift_right_logical(slot, position), position + 1)
    low = lax.bitwise_and(slot, (1 << position) - 1)
    return high + low + bit * (1 << position)


def shade(item, bit, low_bits, v, samples, levels, splats, out):
    edge, halves = samples.shape[1], samples.shape[2]
    slot, group = item // 2, lax.rem(item, 2)
    unit = spread_bit(slot, low_bits, bit)
    h = lax.rem(unit, halves)
    start = pl.multiple_of((unit // halves) * BC + group * SUB, SUB)
    level = levels[pl.ds(start, SUB), :]
    flip = splats[FLIPS + v]
    ext_slope, ext_shift = splats[EXT_SLOPE], splats[EXT_SHIFT]
    shift = []
    for j in range(4):
        need = j + flip * (3 - 2 * j)
        shift.append(jnp.where(level > need, ext_shift, -1e30))
    clear = jnp.ones((SUB, LANES), jnp.float32)
    sums = [jnp.zeros((SUB, LANES), jnp.float32) for _ in range(3)]
    for k in range(edge):
        s = samples[v, k, h, pl.ds(start, SUB), :]
        passed = jnp.exp2(-jnp.exp2(s * ext_slope + shift[k // (edge // 4)]))
        beyond = clear * passed
        weight = clear - beyond
        clear = beyond
        for c in range(3):
            sums[c] = sums[c] + weight * jnp.tanh(s * splats[SLOPES + c] + splats[SHIFTS + c])
    opacity = 1.0 - clear
    place = pl.multiple_of(group * SUB, SUB)
    for c in range(3):
        out[slot, v, c, pl.ds(place, SUB), :] = (opacity + sums[c]) * 0.5
    out[slot, v, 3, pl.ds(place, SUB), :] = opacity


def wide(ref, *index):
    return jnp.concatenate([ref[(*index, h)] for h in range(ref.shape[len(index)])], axis=-1)


def to_slices(lines, r, perm, moved):
    edge, halves = moved.shape[0], moved.shape[1]
    x = jnp.concatenate([lines[r, h].reshape(BC * edge, LANES) for h in range(halves)], axis=-1)
    slices = jnp.dot(wide(perm), x, preferred_element_type=jnp.float32).astype(jnp.bfloat16)
    place = r * BC if isinstance(r, int) else pl.multiple_of(r * BC, BC)
    for k in range(edge):
        for h in range(halves):
            moved[k, h, pl.ds(place, BC), :] = slices[k * BC : (k + 1) * BC, h * LANES : (h + 1) * LANES]


def flips_of(splats):
    return [splats[FLIPS + v, 0, 0] > 0.5 for v in range(2)]


def resample(k, v, flips, moved, table, samples):
    edge, halves = samples.shape[1], samples.shape[2]
    result = jnp.dot(wide(moved, k), wide(table, k), preferred_element_type=jnp.float32)
    place = jnp.where(flips[v], edge - 1 - k, k)
    for h in range(halves):
        samples[v, place, h] = result[:, h * LANES : (h + 1) * LANES]


def beside(steps, items, jobs, item_fn, job_fn):
    def body(i, carry):
        for n in range(jobs // steps):
            job_fn(i * (jobs // steps) + n)
        for n in range(items // steps):
            item_fn(i * (items // steps) + n)
        return carry

    lax.fori_loop(0, steps, body, 0)


def first_kernel(
    rounds, low_bits,
    order, cgain, cbias, egain, ebias, cost, bricks, weights0, weights1,
    send, samples, moved1, moved2, lines3, tab0, tab1, perm, levels, splats,
    lines0, lines1, lines2, moved, w0, w1, s_order, s_cgain, s_cbias, v_cost, sems,
):
    me = lax.axis_index("depth")
    rows, edge = lines0.shape[0], moved.shape[0]
    halves = samples.shape[2]
    chunk = rows * BC
    top, second = bit_of(me, rounds - 1), bit_of(me, rounds - 2)
    quarters = [
        (1 - top) * 2 + 1 - second, (1 - top) * 2 + second, top * 2 + 1 - second, top * 2 + second
    ]
    small = [(weights0, w0), (weights1, w1), (order, s_order), (cgain, s_cgain), (cbias, s_cbias), (cost, v_cost)]
    pairs = list(small)
    for quarter, lines in zip(quarters, (lines0, lines1, lines2, lines3)):
        for h in range(halves):
            span = pl.ds(h * LANES, LANES)
            pairs.append((bricks.at[pl.ds(quarter * rows, rows), :, :, span], lines.at[:, h]))
    copies = [pltpu.make_async_copy(a, b, sems.at[i]) for i, (a, b) in enumerate(pairs)]
    for copy in copies:
        copy.start()
    ready = [copies[len(small) + q * halves : len(small) + (q + 1) * halves] for q in range(4)]

    size = BC * edge
    for h in range(halves):
        out_row = lax.broadcasted_iota(jnp.int32, (size, LANES), 0)
        in_row = lax.broadcasted_iota(jnp.int32, (size, LANES), 1) + h * LANES
        wanted = lax.rem(out_row, BC) * edge + out_row // BC
        perm[h] = jnp.where(wanted == in_row, 1.0, 0.0).astype(jnp.bfloat16)

    for copy in copies[: len(small)]:
        copy.wait()

    def splat(value):
        return jnp.full((SUB, LANES), value, jnp.float32)

    splats[EXT_SLOPE] = splat(egain[0] * LOG2E)
    splats[EXT_SHIFT] = splat(ebias[0] * LOG2E + math.log2(LOG2E))
    for c in range(3):
        splats[SLOPES + c] = splat(s_cgain[c] * 0.5)
        splats[SHIFTS + c] = splat(s_cbias[c] * 0.5)
    flips = []
    for v in range(2):
        flips.append(s_order[v, 0] > s_order[v, order.shape[1] - 1])
        splats[FLIPS + v] = splat(jnp.where(flips[v], 1.0, 0.0))
        rank = lax.bitwise_xor(me, s_order[v, 0])
        for bit in range(rounds):
            splats[FRONTS + v * rounds + bit] = splat(bit_of(rank, bit).astype(jnp.float32))

    total = v_cost.shape[1]
    here = lax.broadcasted_iota(jnp.int32, (chunk, total), 0)
    there = lax.broadcasted_iota(jnp.int32, (chunk, total), 1)
    row = v_cost[...].astype(jnp.float32)
    ones = jnp.ones((total, LANES), jnp.bfloat16)
    for i, quarter in enumerate(quarters):
        picked = jnp.where(here + quarter * chunk == there, row, 0.0).astype(jnp.bfloat16)
        levels[i] = jnp.dot(picked, ones, preferred_element_type=jnp.float32)

    tile = LANES // edge
    lane = lax.broadcasted_iota(jnp.int32, (edge, LANES), 1)
    source = lax.broadcasted_iota(jnp.int32, (edge, LANES), 0)
    masks = [jnp.where(lane // edge == (-y) % tile, 1.0, 0.0) for y in range(tile)]
    column = jnp.where(lax.rem(lane, edge) == source, 1.0, 0.0)
    blank = jnp.zeros((edge, LANES), jnp.bfloat16)

    def build(k, carry):
        cols = w0[k]
        blocks = [(cols * masks[y]).astype(jnp.bfloat16) for y in range(tile)]
        for y in range(edge):
            for h in range(halves):
                span = pl.ds(y * edge, edge)
                tab0[k, h, span, :] = blocks[y % tile] if y // tile == h else blank
                tab1[k, h, span, :] = (column * w1[k, h, y : y + 1, :]).astype(jnp.bfloat16)
        return carry

    lax.fori_loop(0, edge, build, 0)

    for copy in ready[0]:
        copy.wait()
    for r in range(rows):
        to_slices(lines0, r, perm, moved)
    for k in range(edge):
        resample(k, 0, flips, moved, tab0, samples)

    mine = bit_of(me, 0)

    def item(v):
        return lambda i: shade(i, 1 - mine, low_bits, v, samples, levels.at[0], splats, send)

    count = chunk // SUB * halves // 2
    beside(2, count, edge, item(0), lambda k: resample(k, 1, flips, moved, tab1, samples))
    for copy in ready[1] + ready[2]:
        copy.wait()

    def slices(r):
        to_slices(lines1, r, perm, moved1)
        to_slices(lines2, r, perm, moved2)

    beside(2, count, rows, item(1), slices)
    for copy in ready[3]:
        copy.wait()


def second_kernel(low_bits, samples, moved_next, tab0, tab1, levels, splats, kept, samples_next):
    mine = bit_of(lax.axis_index("depth"), 0)
    edge = samples.shape[1]
    count = samples.shape[3] // SUB * samples.shape[2] // 2
    flips = flips_of(splats)
    for v, table in enumerate((tab0, tab1)):
        beside(
            2, count, edge,
            lambda i: shade(i, mine, low_bits, v, samples, levels.at[0], splats, kept),
            lambda k: resample(k, v, flips, moved_next, table, samples_next),
        )


def quarter_kernel(low_bits, index, *refs):
    levels, splats, samples, *refs = refs
    if index == 1:
        moved, tab0, tab1, lines, perm, send, kept, samples_next, moved_next = refs
    elif index == 2:
        moved, tab0, tab1, send, kept, samples_next = refs
    else:
        send, kept = refs
    mine = bit_of(lax.axis_index("depth"), 0)
    edge = samples.shape[1]
    count = samples.shape[3] // SUB * samples.shape[2] // 2
    rows = samples.shape[3] // BC
    flips = flips_of(splats)
    for v in range(2):

        def items(i):
            shade(i, 1 - mine, low_bits, v, samples, levels.at[index], splats, send)
            shade(i, mine, low_bits, v, samples, levels.at[index], splats, kept)

        def jobs(r):
            for n in range(edge // rows):
                resample(r * (edge // rows) + n, v, flips, moved, tab1 if v else tab0, samples_next)
            if index == 1 and v == 0:
                to_slices(lines, r, perm, moved_next)

        beside(rows, count, rows if index < 3 else 0, items, jobs)


VMEM = pl.BlockSpec(memory_space=pltpu.VMEM)
HBM = pl.BlockSpec(memory_space=pltpu.HBM)


def call(kernel, ins, outs, cycles, scratch=(), limit=4 << 20, specs=None):
    outs = tuple(jax.ShapeDtypeStruct(shape, dtype) for shape, dtype in outs)
    return pl.pallas_call(
        kernel,
        out_shape=outs,
        in_specs=specs or [VMEM] * len(ins),
        out_specs=tuple(VMEM for _ in outs),
        scratch_shapes=list(scratch),
        compiler_params=pltpu.CompilerParams(vmem_limit_bytes=limit),
        cost_estimate=pl.CostEstimate(flops=cycles * 4096, bytes_accessed=1 << 18, transcendentals=0),
    )(*ins)


def render(rounds, low_bits, order, cgain, cbias, egain, ebias, cost, bricks, weights0, weights1):
    total, edge, plane = bricks.shape
    rows = total // BC // 4
    chunk, halves, size = rows * BC, plane // LANES, BC * edge
    f32, bf16 = jnp.float32, jnp.bfloat16
    part = ((rows * halves // 2, 2, 4, BC, LANES), f32)
    samples = ((2, edge, halves, chunk, LANES), f32)
    lines = ((rows, halves, BC, edge, LANES), bf16)
    moved = ((edge, halves, chunk, LANES), bf16)
    table = ((edge, halves, plane, LANES), bf16)
    square = ((size // LANES, size, LANES), bf16)
    levels = ((4, chunk, LANES), f32)
    splats = ((FRONTS + 2 * rounds, SUB, LANES), f32)
    bricks = bricks.reshape(total // BC, BC, edge, plane)
    far = lambda x: pltpu.with_memory_space_constraint(x, pltpu.HBM)
    ins = (far(order), far(cgain), far(cbias), egain, ebias, far(cost), far(bricks), far(weights0), far(weights1))
    specs = [HBM] * 3 + [pl.BlockSpec(memory_space=pltpu.SMEM)] * 2 + [HBM] * 4
    send0, samples0, moved1, moved2, lines3, tab0, tab1, perm, levels_, splats_ = call(
        functools.partial(first_kernel, rounds, low_bits), ins,
        (part, samples, moved, moved, lines, table, table, square, levels, splats), 4000,
        [pltpu.VMEM(*lines), pltpu.VMEM(*lines), pltpu.VMEM(*lines), pltpu.VMEM(*moved),
         pltpu.VMEM(weights0.shape, f32), pltpu.VMEM(weights1.shape, f32),
         pltpu.SMEM(order.shape, order.dtype), pltpu.SMEM(cgain.shape, f32), pltpu.SMEM(cbias.shape, f32),
         pltpu.VMEM(cost.shape, cost.dtype), pltpu.SemaphoreType.DMA((6 + 4 * halves,))],
        20 << 20, specs,
    )
    kept0, samples1 = call(
        functools.partial(second_kernel, low_bits),
        (samples0, moved1, tab0, tab1, levels_, splats_), (part, samples), 1800, (), 14 << 20,
    )
    send1, kept1, samples2, moved3 = call(
        functools.partial(quarter_kernel, low_bits, 1),
        (levels_, splats_, samples1, moved2, tab0, tab1, lines3, perm), (part, part, samples, moved), 3500, (), 14 << 20,
    )
    send2, kept2, samples3 = call(
        functools.partial(quarter_kernel, low_bits, 2),
        (levels_, splats_, samples2, moved3, tab0, tab1), (part, part, samples), 3500, (), 14 << 20,
    )
    send3, kept3 = call(
        functools.partial(quarter_kernel, low_bits, 3),
        (levels_, splats_, samples3), (part, part), 3300, (), 8 << 20,
    )
    return splats_, [(send0, kept0), (send1, kept1), (send2, kept2), (send3, kept3)]


def merged_pair(front, kept, incoming):
    behind = 1.0 - front * incoming[3]
    ahead = 1.0 - (1.0 - front) * kept[3]
    return [kept[c] * behind + incoming[c] * ahead for c in range(4)]


def front_of(splats, v, rounds, bit):
    one = splats[FRONTS + v * rounds + bit]
    return jnp.concatenate([one] * (BC // SUB), axis=0)


def read(ref, unit, v):
    parts = [ref[unit, v, c] for c in range(4)]
    return [decode(x) for x in parts] if ref.dtype == jnp.int16 else parts


def merge_kernel(rounds, bit, many, low_bits, splats, kept, *refs):
    incoming, outs = refs[:many], refs[many:]
    mine = bit_of(lax.axis_index("depth"), bit + many)
    units = kept.shape[0]
    for v in range(2):
        for i, out in enumerate(outs):
            for slot in range(units // len(outs)):
                unit = slot
                if len(outs) > 1:
                    unit = spread_bit(slot, low_bits, 1 - mine if i == 0 else mine)
                done = read(kept, unit, v)
                for n, came in enumerate(incoming):
                    done = merged_pair(front_of(splats, v, rounds, bit + n), done, read(came, unit, v))
                for c in range(4):
                    out[slot, v, c] = encode(done[c]) if out.dtype == jnp.int16 else done[c]


def merge(rounds, bit, low_bits, types, splats, kept, incoming):
    units, tail = kept.shape[0], kept.shape[1:]
    outs = tuple(((units // len(types), *tail), t) for t in types)
    kernel = functools.partial(merge_kernel, rounds, bit, len(incoming), low_bits)
    return call(kernel, (splats, kept, *incoming), outs, 300)


def finish_kernel(rounds, bit, edge, splats, kept, *refs):
    incoming, out = refs[:-1], refs[-1]
    chunks = LANES // edge
    chunk_of = lax.broadcasted_iota(jnp.int32, (SUB, LANES), 1) // edge
    for v in range(2):
        for unit in range(kept.shape[0]):
            done = read(kept, unit, v)
            for n, came in enumerate(incoming):
                done = merged_pair(front_of(splats, v, rounds, bit + n), done, read(came, unit, v))
            for c in range(4):
                for g in range(BC // SUB):
                    x = done[c][g * SUB : (g + 1) * SUB, :]
                    x = pltpu.roll(x, 0, 1, stride=edge, stride_axis=0)
                    for step in range(3):
                        turned = pltpu.roll(x, SUB - (1 << step), 0)
                        x = jnp.where(bit_of(chunk_of, step) == 1, turned, x)
                    x = pltpu.roll(x, 0, 1, stride=edge, stride_axis=0)
                    out[v, c, unit * chunks : (unit + 1) * chunks, g * LANES : (g + 1) * LANES] = x


def finish(rounds, bit, edge, splats, kept, incoming):
    units = kept.shape[0]
    out = ((2, 4, units * LANES // edge, BC * edge), jnp.float32)
    return call(functools.partial(finish_kernel, rounds, bit, edge), (splats, kept, *incoming), (out,), 1500)[0]


def swapped(x, bit):
    count = lax.axis_size("depth")
    return lax.ppermute(x, "depth", [(i, i ^ 1 << bit) for i in range(count)])


def shards(bricks, cost, order, color_gain, color_bias, ext_gain, ext_bias):
    bricks = bricks[0]
    total, edge, plane = bricks.shape
    count = lax.axis_size("depth")
    rounds = count.bit_length() - 1
    units = total // BC * (plane // LANES)
    low_bits = (units // count).bit_length() - 1
    weights0, weights1 = (jnp.asarray(t) for t in shear_weights(edge))
    splats, parts = render(
        rounds, low_bits, order, color_gain, color_bias, ext_gain, ext_bias, cost, bricks, weights0, weights1
    )
    f32, i16 = jnp.float32, jnp.int16
    near = rounds - 2

    def close(index):
        send, kept = parts[index]
        for bit in range(near - 1):
            incoming = swapped(send, bit)
            send, kept = merge(rounds, bit, low_bits, (f32, f32), splats, kept, [incoming])
        return kept, swapped(send, near - 1)

    def leave(index):
        kept, incoming = close(index)
        (done,) = merge(rounds, near - 1, low_bits, (i16,), splats, kept, [incoming])
        return swapped(done, near)

    across = leave(0)
    kept, incoming = close(1)
    (done,) = merge(rounds, near - 1, low_bits, (i16,), splats, kept, [incoming, across])
    top = swapped(done, near + 1)
    across = leave(2)
    kept, incoming = close(3)
    return finish(rounds, near - 1, edge, splats, kept, [incoming, across, top])


def solution(mesh):
    in_specs = (P("depth", "image", None, None), P("depth", "image"), P(), P(), P(), P(), P())
    out_specs = P(None, None, "depth", "image")

    return jax.shard_map(shards, mesh=mesh, in_specs=in_specs, out_specs=out_specs, check_vma=False)
```

```python
import functools
import math

import jax
import jax.numpy as jnp
from jax import lax
from jax.experimental import pallas as pl
from jax.experimental.pallas import tpu as pltpu
from jax.sharding import PartitionSpec as P


BC = 16
LANES = 128
SUB = 8
SHEAR = (0.45, -0.3)
LOG2E = 1.0 / math.log(2.0)

CODE_RANGE = 32.0
CODE_STEP = 2047.0
CODE_BIAS = 32768.0


def encode(x):
    logs = jnp.log(jnp.maximum(x, 2.0**-CODE_RANGE))
    code = logs * (CODE_STEP * LOG2E) + (CODE_RANGE * CODE_STEP + 0.5)
    return (code.astype(jnp.int32) - int(CODE_BIAS)).astype(jnp.int16)


def decode(code):
    value = code.astype(jnp.int32).astype(jnp.float32)
    return jnp.exp2(value * (1.0 / CODE_STEP) + (CODE_BIAS / CODE_STEP - CODE_RANGE))


EXT_SLOPE, EXT_SHIFT, SLOPES, SHIFTS, FLIPS, FRONTS = 0, 1, 2, 5, 8, 10


def bit_of(value, bit):
    return lax.bitwise_and(lax.shift_right_logical(value, bit), 1)


def spread_bit(slot, position, bit):
    high = lax.shift_left(lax.shift_right_logical(slot, position), position + 1)
    low = lax.bitwise_and(slot, (1 << position) - 1)
    return high + low + bit * (1 << position)


def shade(item, bit, low_bits, v, samples, levels, splats, out):
    edge, halves = samples[v].shape[0], samples[v].shape[1]
    slot, group = item // 2, lax.rem(item, 2)
    unit = spread_bit(slot, low_bits, bit)
    h = lax.rem(unit, halves)
    start = pl.multiple_of((unit // halves) * BC + group * SUB, SUB)
    level = levels[pl.ds(start, SUB), :]
    flip = splats[FLIPS + v]
    ext_slope, ext_shift = splats[EXT_SLOPE], splats[EXT_SHIFT]
    shift = []
    for j in range(4):
        need = j + flip * (3 - 2 * j)
        shift.append(jnp.where(level > need, ext_shift, -1e30))
    clear = jnp.ones((SUB, LANES), jnp.float32)
    depth = jnp.zeros((SUB, LANES), jnp.float32)
    sums = [jnp.zeros((SUB, LANES), jnp.float32) for _ in range(3)]
    for k in range(edge):
        s = samples[v][k, h, pl.ds(start, SUB), :]
        depth = depth - jnp.exp2(s * ext_slope + shift[k // (edge // 4)])
        beyond = jnp.exp2(depth)
        weight = clear - beyond
        clear = beyond
        for c in range(3):
            sums[c] = sums[c] + weight * jnp.tanh(s * splats[SLOPES + c] + splats[SHIFTS + c])
    opacity = 1.0 - clear
    place = pl.multiple_of(group * SUB, SUB)
    for c in range(3):
        out[slot, v, c, pl.ds(place, SUB), :] = (opacity + sums[c]) * 0.5
    out[slot, v, 3, pl.ds(place, SUB), :] = opacity


def wide(ref, *index):
    return jnp.concatenate([ref[(*index, h)] for h in range(ref.shape[len(index)])], axis=-1)


def to_slices(lines, r, perm, moved):
    edge, halves = moved.shape[0], moved.shape[1]
    x = jnp.concatenate([lines[r, h].reshape(BC * edge, LANES) for h in range(halves)], axis=-1)
    slices = jnp.dot(wide(perm), x, preferred_element_type=jnp.float32).astype(jnp.bfloat16)
    place = r * BC if isinstance(r, int) else pl.multiple_of(r * BC, BC)
    for k in range(edge):
        for h in range(halves):
            moved[k, h, pl.ds(place, BC), :] = slices[k * BC : (k + 1) * BC, h * LANES : (h + 1) * LANES]


def flips_of(splats):
    return [splats[FLIPS + v, 0, 0] > 0.5 for v in range(2)]


def resample(k, v, flips, moved, table, samples):
    edge, halves = samples[v].shape[0], samples[v].shape[1]
    result = jnp.dot(wide(moved, k), wide(table, k), preferred_element_type=jnp.float32)
    place = jnp.where(flips[v], edge - 1 - k, k)
    for h in range(halves):
        samples[v][place, h] = result[:, h * LANES : (h + 1) * LANES]


def beside(steps, items, jobs, item_fn, job_fn):
    def body(i, carry):
        for n in range(jobs // steps):
            job_fn(i * (jobs // steps) + n)
        for n in range(items // steps):
            item_fn(i * (items // steps) + n)
        return carry

    lax.fori_loop(0, steps, body, 0)


def first_kernel(
    rounds, low_bits,
    order, cgain, cbias, egain, ebias, cost, bricks,
    send, samples0, samples1, moved1, moved2, lines3, tab0, tab1, perm, levels, splats,
    lines0, lines1, lines2, moved, s_order, s_cgain, s_cbias, v_cost, sems,
):
    me = lax.axis_index("depth")
    rows, edge = lines0.shape[0], moved.shape[0]
    samples = (samples0, samples1)
    halves = samples0.shape[1]
    chunk = rows * BC
    top, second = bit_of(me, rounds - 1), bit_of(me, rounds - 2)
    quarters = [
        (1 - top) * 2 + 1 - second, (1 - top) * 2 + second, top * 2 + 1 - second, top * 2 + second
    ]
    small = [(order, s_order), (cgain, s_cgain), (cbias, s_cbias), (cost, v_cost)]
    pairs = list(small)
    for quarter, lines in zip(quarters, (lines0, lines1, lines2, lines3)):
        for h in range(halves):
            span = pl.ds(h * LANES, LANES)
            pairs.append((bricks.at[pl.ds(quarter * rows, rows), :, :, span], lines.at[:, h]))
    copies = [pltpu.make_async_copy(a, b, sems.at[i]) for i, (a, b) in enumerate(pairs)]
    for copy in copies:
        copy.start()
    ready = [copies[len(small) + q * halves : len(small) + (q + 1) * halves] for q in range(4)]

    size = BC * edge
    for h in range(halves):
        out_row = lax.broadcasted_iota(jnp.int32, (size, LANES), 0)
        in_row = lax.broadcasted_iota(jnp.int32, (size, LANES), 1) + h * LANES
        wanted = lax.rem(out_row, BC) * edge + out_row // BC
        perm[h] = jnp.where(wanted == in_row, 1.0, 0.0).astype(jnp.bfloat16)

    tile = LANES // edge
    lane = lax.broadcasted_iota(jnp.int32, (edge, LANES), 1)
    source = lax.broadcasted_iota(jnp.int32, (edge, LANES), 0)
    masks = [jnp.where(lane // edge == (-y) % tile, 1.0, 0.0) for y in range(tile)]
    same_column = lax.rem(lane, edge) == source
    blank = jnp.zeros((edge, LANES), jnp.bfloat16)
    target_col = lax.rem(lane, edge).astype(jnp.float32)
    target_row = [(lax.rem(tile - lane // edge, tile) + h * tile).astype(jnp.float32) for h in range(halves)]
    source = source.astype(jnp.float32)

    def taps(target, view, k):
        position = target + SHEAR[view] * (k.astype(jnp.float32) - (edge - 1) / 2.0)
        anchor = jnp.floor(position)
        high = position - anchor
        return anchor, 1.0 - high, high

    def weigh(source, anchor, low, high):
        return jnp.where(source == anchor, low, 0.0) + jnp.where(source == anchor + 1.0, high, 0.0)

    def build(k, carry):
        cols = weigh(source, *taps(target_col, 0, k))
        blocks = [(cols * masks[y]).astype(jnp.bfloat16) for y in range(tile)]
        lines = []
        for h in range(halves):
            anchor, low, high = taps(target_row[h], 1, k)
            lines.append((anchor, jnp.where(same_column, low, 0.0), jnp.where(same_column, high, 0.0)))
        for y in range(edge):
            for h in range(halves):
                span = pl.ds(y * edge, edge)
                tab0[k, h, span, :] = blocks[y % tile] if y // tile == h else blank
                tab1[k, h, span, :] = weigh(float(y), *lines[h]).astype(jnp.bfloat16)
        return carry

    lax.fori_loop(0, edge, build, 0)

    for copy in copies[: len(small)]:
        copy.wait()

    def splat(value):
        return jnp.full((SUB, LANES), value, jnp.float32)

    splats[EXT_SLOPE] = splat(egain[0] * LOG2E)
    splats[EXT_SHIFT] = splat(ebias[0] * LOG2E + math.log2(LOG2E))
    for c in range(3):
        splats[SLOPES + c] = splat(s_cgain[c] * 0.5)
        splats[SHIFTS + c] = splat(s_cbias[c] * 0.5)
    flips = []
    for v in range(2):
        flips.append(s_order[v, 0] > s_order[v, order.shape[1] - 1])
        splats[FLIPS + v] = splat(jnp.where(flips[v], 1.0, 0.0))
        rank = lax.bitwise_xor(me, s_order[v, 0])
        for bit in range(rounds):
            splats[FRONTS + v * rounds + bit] = splat(bit_of(rank, bit).astype(jnp.float32))

    total = v_cost.shape[1]
    here = lax.broadcasted_iota(jnp.int32, (chunk, total), 0)
    there = lax.broadcasted_iota(jnp.int32, (chunk, total), 1)
    row = v_cost[...].astype(jnp.float32)
    ones = jnp.ones((total, LANES), jnp.bfloat16)
    for i, quarter in enumerate(quarters):
        picked = jnp.where(here + quarter * chunk == there, row, 0.0).astype(jnp.bfloat16)
        levels[i] = jnp.dot(picked, ones, preferred_element_type=jnp.float32)

    for copy in ready[0]:
        copy.wait()
    for r in range(rows):
        to_slices(lines0, r, perm, moved)
    for k in range(edge):
        resample(k, 0, flips, moved, tab0, samples)

    mine = bit_of(me, 0)

    def item(v):
        return lambda i: shade(i, 1 - mine, low_bits, v, samples, levels.at[0], splats, send)

    count = chunk // SUB * halves // 2
    beside(2, count, edge, item(0), lambda k: resample(k, 1, flips, moved, tab1, samples))
    for copy in ready[1] + ready[2]:
        copy.wait()

    def slices(r):
        to_slices(lines1, r, perm, moved1)
        to_slices(lines2, r, perm, moved2)

    beside(2, count, rows, item(1), slices)
    for copy in ready[3]:
        copy.wait()


def second_kernel(low_bits, here0, here1, moved_next, tab0, tab1, levels, splats, kept, next0, next1):
    mine = bit_of(lax.axis_index("depth"), 0)
    samples, samples_next = (here0, here1), (next0, next1)
    edge, halves, chunk, _ = here0.shape
    count = chunk // SUB * halves // 2
    flips = flips_of(splats)
    for v, table in enumerate((tab0, tab1)):
        beside(
            2, count, edge,
            lambda i: shade(i, mine, low_bits, v, samples, levels.at[0], splats, kept),
            lambda k: resample(k, v, flips, moved_next, table, samples_next),
        )


def quarter_kernel(low_bits, index, *refs):
    levels, splats, here0, here1, *refs = refs
    samples = (here0, here1)
    if index == 1:
        moved, tab0, tab1, lines, perm, send, kept, *samples_next, moved_next = refs
    elif index == 2:
        moved, tab0, tab1, send, kept, *samples_next = refs
    else:
        send, kept = refs
    mine = bit_of(lax.axis_index("depth"), 0)
    edge, halves, chunk, _ = here0.shape
    count = chunk // SUB * halves // 2
    rows = chunk // BC
    flips = flips_of(splats)
    for v in range(2):

        def items(i):
            shade(i, 1 - mine, low_bits, v, samples, levels.at[index], splats, send)
            shade(i, mine, low_bits, v, samples, levels.at[index], splats, kept)

        def jobs(r):
            for n in range(edge // rows):
                resample(r * (edge // rows) + n, v, flips, moved, tab1 if v else tab0, samples_next)
            if index == 1 and v == 0:
                to_slices(lines, r, perm, moved_next)

        beside(rows, count, rows if index < 3 else 0, items, jobs)


VMEM = pl.BlockSpec(memory_space=pltpu.VMEM)
HBM = pl.BlockSpec(memory_space=pltpu.HBM)


def call(kernel, ins, outs, cycles, scratch=(), limit=4 << 20, specs=None):
    outs = tuple(jax.ShapeDtypeStruct(shape, dtype) for shape, dtype in outs)
    return pl.pallas_call(
        kernel,
        out_shape=outs,
        in_specs=specs or [VMEM] * len(ins),
        out_specs=tuple(VMEM for _ in outs),
        scratch_shapes=list(scratch),
        compiler_params=pltpu.CompilerParams(vmem_limit_bytes=limit),
        cost_estimate=pl.CostEstimate(flops=cycles * 4096, bytes_accessed=1 << 18, transcendentals=0),
    )(*ins)


def render(rounds, low_bits, order, cgain, cbias, egain, ebias, cost, bricks):
    total, edge, plane = bricks.shape
    rows = total // BC // 4
    chunk, halves, size = rows * BC, plane // LANES, BC * edge
    f32, bf16 = jnp.float32, jnp.bfloat16
    part = ((rows * halves // 2, 2, 4, BC, LANES), f32)
    samples = ((edge, halves, chunk, LANES), f32)
    lines = ((rows, halves, BC, edge, LANES), bf16)
    moved = ((edge, halves, chunk, LANES), bf16)
    table = ((edge, halves, plane, LANES), bf16)
    square = ((size // LANES, size, LANES), bf16)
    levels = ((4, chunk, LANES), f32)
    splats = ((FRONTS + 2 * rounds, SUB, LANES), f32)
    bricks = bricks.reshape(total // BC, BC, edge, plane)
    far = lambda x: pltpu.with_memory_space_constraint(x, pltpu.HBM)
    ins = (far(order), far(cgain), far(cbias), egain, ebias, far(cost), far(bricks))
    specs = [HBM] * 3 + [pl.BlockSpec(memory_space=pltpu.SMEM)] * 2 + [HBM] * 2
    send0, *samples0, moved1, moved2, lines3, tab0, tab1, perm, levels_, splats_ = call(
        functools.partial(first_kernel, rounds, low_bits), ins,
        (part, samples, samples, moved, moved, lines, table, table, square, levels, splats), 4000,
        [pltpu.VMEM(*lines), pltpu.VMEM(*lines), pltpu.VMEM(*lines), pltpu.VMEM(*moved),
         pltpu.SMEM(order.shape, order.dtype), pltpu.SMEM(cgain.shape, f32), pltpu.SMEM(cbias.shape, f32),
         pltpu.VMEM(cost.shape, cost.dtype), pltpu.SemaphoreType.DMA((4 + 4 * halves,))],
        20 << 20, specs,
    )
    kept0, *samples1 = call(
        functools.partial(second_kernel, low_bits),
        (*samples0, moved1, tab0, tab1, levels_, splats_), (part, samples, samples), 1800, (), 14 << 20,
    )
    send1, kept1, *samples2, moved3 = call(
        functools.partial(quarter_kernel, low_bits, 1),
        (levels_, splats_, *samples1, moved2, tab0, tab1, lines3, perm), (part, part, samples, samples, moved), 3500, (), 14 << 20,
    )
    send2, kept2, *samples3 = call(
        functools.partial(quarter_kernel, low_bits, 2),
        (levels_, splats_, *samples2, moved3, tab0, tab1), (part, part, samples, samples), 3500, (), 14 << 20,
    )
    send3, kept3 = call(
        functools.partial(quarter_kernel, low_bits, 3),
        (levels_, splats_, *samples3), (part, part), 3300, (), 8 << 20,
    )
    return splats_, [(send0, kept0), (send1, kept1), (send2, kept2), (send3, kept3)]


def merged_pair(front, kept, incoming):
    behind = 1.0 - front * incoming[3]
    ahead = 1.0 - (1.0 - front) * kept[3]
    return [kept[c] * behind + incoming[c] * ahead for c in range(4)]


def front_of(splats, v, rounds, bit):
    one = splats[FRONTS + v * rounds + bit]
    return jnp.concatenate([one] * (BC // SUB), axis=0)


def read(ref, unit, v):
    parts = [ref[unit, v, c] for c in range(4)]
    return [decode(x) for x in parts] if ref.dtype == jnp.int16 else parts


def merge_kernel(rounds, bit, many, low_bits, splats, kept, *refs):
    incoming, outs = refs[:many], refs[many:]
    mine = bit_of(lax.axis_index("depth"), bit + many)
    units = kept.shape[0]
    for v in range(2):
        for i, out in enumerate(outs):
            for slot in range(units // len(outs)):
                unit = slot
                if len(outs) > 1:
                    unit = spread_bit(slot, low_bits, 1 - mine if i == 0 else mine)
                done = read(kept, unit, v)
                for n, came in enumerate(incoming):
                    done = merged_pair(front_of(splats, v, rounds, bit + n), done, read(came, unit, v))
                for c in range(4):
                    out[slot, v, c] = encode(done[c]) if out.dtype == jnp.int16 else done[c]


def merge(rounds, bit, low_bits, types, splats, kept, incoming):
    units, tail = kept.shape[0], kept.shape[1:]
    outs = tuple(((units // len(types), *tail), t) for t in types)
    kernel = functools.partial(merge_kernel, rounds, bit, len(incoming), low_bits)
    return call(kernel, (splats, kept, *incoming), outs, 300)


def finish_kernel(rounds, bit, edge, splats, kept, *refs):
    incoming, out = refs[:-1], refs[-1]
    chunks = LANES // edge
    chunk_of = lax.broadcasted_iota(jnp.int32, (SUB, LANES), 1) // edge
    for v in range(2):
        for unit in range(kept.shape[0]):
            done = read(kept, unit, v)
            for n, came in enumerate(incoming):
                done = merged_pair(front_of(splats, v, rounds, bit + n), done, read(came, unit, v))
            for c in range(4):
                for g in range(BC // SUB):
                    x = done[c][g * SUB : (g + 1) * SUB, :]
                    x = pltpu.roll(x, 0, 1, stride=edge, stride_axis=0)
                    for step in range(3):
                        turned = pltpu.roll(x, SUB - (1 << step), 0)
                        x = jnp.where(bit_of(chunk_of, step) == 1, turned, x)
                    x = pltpu.roll(x, 0, 1, stride=edge, stride_axis=0)
                    out[v, c, unit * chunks : (unit + 1) * chunks, g * LANES : (g + 1) * LANES] = x


def finish(rounds, bit, edge, splats, kept, incoming):
    units = kept.shape[0]
    out = ((2, 4, units * LANES // edge, BC * edge), jnp.float32)
    return call(functools.partial(finish_kernel, rounds, bit, edge), (splats, kept, *incoming), (out,), 1500)[0]


def swapped(x, bit):
    count = lax.axis_size("depth")
    return lax.ppermute(x, "depth", [(i, i ^ 1 << bit) for i in range(count)])


def shards(bricks, cost, order, color_gain, color_bias, ext_gain, ext_bias):
    bricks = bricks[0]
    total, edge, plane = bricks.shape
    count = lax.axis_size("depth")
    rounds = count.bit_length() - 1
    units = total // BC * (plane // LANES)
    low_bits = (units // count).bit_length() - 1
    splats, parts = render(
        rounds, low_bits, order, color_gain, color_bias, ext_gain, ext_bias, cost, bricks
    )
    f32, i16 = jnp.float32, jnp.int16
    near = rounds - 2

    def close(index):
        send, kept = parts[index]
        for bit in range(near - 1):
            incoming = swapped(send, bit)
            send, kept = merge(rounds, bit, low_bits, (f32, f32), splats, kept, [incoming])
        return kept, swapped(send, near - 1)

    def leave(index):
        kept, incoming = close(index)
        (done,) = merge(rounds, near - 1, low_bits, (i16,), splats, kept, [incoming])
        return swapped(done, near)

    across = leave(0)
    kept, incoming = close(1)
    (done,) = merge(rounds, near - 1, low_bits, (i16,), splats, kept, [incoming, across])
    top = swapped(done, near + 1)
    across = leave(2)
    kept, incoming = close(3)
    return finish(rounds, near - 1, edge, splats, kept, [incoming, across, top])


def solution(mesh):
    in_specs = (P("depth", "image", None, None), P("depth", "image"), P(), P(), P(), P(), P())
    out_specs = P(None, None, "depth", "image")

    return jax.shard_map(shards, mesh=mesh, in_specs=in_specs, out_specs=out_specs, check_vma=False)
```

```python
import functools
import math

import jax
import jax.numpy as jnp
from jax import lax
from jax.experimental import pallas as pl
from jax.experimental.pallas import tpu as pltpu
from jax.sharding import PartitionSpec as P


BC = 16
LANES = 128
SUB = 8
SHEAR = (0.45, -0.3)
LOG2E = 1.0 / math.log(2.0)

CODE_RANGE = 32.0
CODE_STEP = 2047.0
CODE_BIAS = 32768.0


def encode(x):
    logs = jnp.log(jnp.maximum(x, 2.0**-CODE_RANGE))
    code = logs * (CODE_STEP * LOG2E) + (CODE_RANGE * CODE_STEP + 0.5)
    return (code.astype(jnp.int32) - int(CODE_BIAS)).astype(jnp.int16)


def decode(code):
    value = code.astype(jnp.int32).astype(jnp.float32)
    return jnp.exp2(value * (1.0 / CODE_STEP) + (CODE_BIAS / CODE_STEP - CODE_RANGE))


EXT_SLOPE, EXT_SHIFT, SLOPES, SHIFTS, FLIPS, FRONTS = 0, 1, 2, 5, 8, 10


def bit_of(value, bit):
    return lax.bitwise_and(lax.shift_right_logical(value, bit), 1)


def spread_bit(slot, position, bit):
    high = lax.shift_left(lax.shift_right_logical(slot, position), position + 1)
    low = lax.bitwise_and(slot, (1 << position) - 1)
    return high + low + bit * (1 << position)


def shade(item, bit, low_bits, v, samples, levels, splats, out):
    edge, halves = samples[v].shape[0], samples[v].shape[1]
    slot, group = item // 2, lax.rem(item, 2)
    unit = spread_bit(slot, low_bits, bit)
    h = lax.rem(unit, halves)
    start = pl.multiple_of((unit // halves) * BC + group * SUB, SUB)
    level = levels[pl.ds(start, SUB), :]
    flip = splats[FLIPS + v]
    ext_slope, ext_shift = splats[EXT_SLOPE], splats[EXT_SHIFT]
    shift = []
    for j in range(4):
        need = j + flip * (3 - 2 * j)
        shift.append(jnp.where(level > need, ext_shift, -1e30))
    clear = jnp.ones((SUB, LANES), jnp.float32)
    depth = jnp.zeros((SUB, LANES), jnp.float32)
    sums = [jnp.zeros((SUB, LANES), jnp.float32) for _ in range(3)]
    for k in range(edge):
        s = samples[v][k, h, pl.ds(start, SUB), :]
        depth = depth - jnp.exp2(s * ext_slope + shift[k // (edge // 4)])
        beyond = jnp.exp2(depth)
        weight = clear - beyond
        clear = beyond
        for c in range(3):
            sums[c] = sums[c] + weight * jnp.tanh(s * splats[SLOPES + c] + splats[SHIFTS + c])
    opacity = 1.0 - clear
    place = pl.multiple_of(group * SUB, SUB)
    for c in range(3):
        out[slot, v, c, pl.ds(place, SUB), :] = (opacity + sums[c]) * 0.5
    out[slot, v, 3, pl.ds(place, SUB), :] = opacity


def wide(ref, *index):
    return jnp.concatenate([ref[(*index, h)] for h in range(ref.shape[len(index)])], axis=-1)


def to_slices(lines, r, perm, moved):
    edge, halves = moved.shape[0], moved.shape[1]
    x = jnp.concatenate([lines[r, h].reshape(BC * edge, LANES) for h in range(halves)], axis=-1)
    slices = jnp.dot(wide(perm), x, preferred_element_type=jnp.float32).astype(jnp.bfloat16)
    place = r * BC if isinstance(r, int) else pl.multiple_of(r * BC, BC)
    for k in range(edge):
        for h in range(halves):
            moved[k, h, pl.ds(place, BC), :] = slices[k * BC : (k + 1) * BC, h * LANES : (h + 1) * LANES]


def flips_of(splats):
    return [splats[FLIPS + v, 0, 0] > 0.5 for v in range(2)]


def resample(k, v, flips, moved, table, samples):
    edge, halves = samples[v].shape[0], samples[v].shape[1]
    result = jnp.dot(wide(moved, k), wide(table, k), preferred_element_type=jnp.float32)
    place = jnp.where(flips[v], edge - 1 - k, k)
    for h in range(halves):
        samples[v][place, h] = result[:, h * LANES : (h + 1) * LANES]


def beside(steps, items, jobs, item_fn, job_fn):
    def body(i, carry):
        for n in range(items // steps):
            item_fn(i * (items // steps) + n)
        for n in range(jobs // steps):
            job_fn(i * (jobs // steps) + n)
        return carry

    lax.fori_loop(0, steps, body, 0)


def first_kernel(
    rounds, low_bits,
    order, cgain, cbias, egain, ebias, cost, bricks,
    send, samples0, samples1, moved1, moved2, moved3, tab0, tab1, levels, splats,
    lines0, lines1, lines2, lines3, perm, moved, s_order, s_cgain, s_cbias, v_cost, sems,
):
    me = lax.axis_index("depth")
    rows, edge = lines0.shape[0], moved.shape[0]
    samples = (samples0, samples1)
    halves = samples0.shape[1]
    chunk = rows * BC
    top, second = bit_of(me, rounds - 1), bit_of(me, rounds - 2)
    quarters = [
        (1 - top) * 2 + 1 - second, top * 2 + 1 - second, (1 - top) * 2 + second, top * 2 + second
    ]
    small = [(order, s_order), (cgain, s_cgain), (cbias, s_cbias), (cost, v_cost)]
    pairs = list(small)
    for quarter, lines in zip(quarters, (lines0, lines1, lines2, lines3)):
        for h in range(halves):
            span = pl.ds(h * LANES, LANES)
            pairs.append((bricks.at[pl.ds(quarter * rows, rows), :, :, span], lines.at[:, h]))
    copies = [pltpu.make_async_copy(a, b, sems.at[i]) for i, (a, b) in enumerate(pairs)]
    early = len(small) + halves
    for copy in copies[:early]:
        copy.start()
    ready = [copies[len(small) + q * halves : len(small) + (q + 1) * halves] for q in range(4)]

    size = BC * edge
    for h in range(halves):
        out_row = lax.broadcasted_iota(jnp.int32, (size, LANES), 0)
        in_row = lax.broadcasted_iota(jnp.int32, (size, LANES), 1) + h * LANES
        wanted = lax.rem(out_row, BC) * edge + out_row // BC
        perm[h] = jnp.where(wanted == in_row, 1.0, 0.0).astype(jnp.bfloat16)

    tile = LANES // edge
    lane = lax.broadcasted_iota(jnp.int32, (edge, LANES), 1)
    source = lax.broadcasted_iota(jnp.int32, (edge, LANES), 0)
    masks = [jnp.where(lane // edge == (-y) % tile, 1.0, 0.0).astype(jnp.bfloat16) for y in range(tile)]
    same_column = lax.rem(lane, edge) == source
    blank = jnp.zeros((edge, LANES), jnp.bfloat16)
    target_col = lax.rem(lane, edge).astype(jnp.float32)
    target_row = [(lax.rem(tile - lane // edge, tile) + h * tile).astype(jnp.float32) for h in range(halves)]
    source = source.astype(jnp.float32)

    def taps(target, view, k):
        position = target + SHEAR[view] * (k.astype(jnp.float32) - (edge - 1) / 2.0)
        anchor = jnp.floor(position)
        high = position - anchor
        return anchor, 1.0 - high, high

    def weigh(source, anchor, low, high):
        return jnp.where(source == anchor, low, 0.0) + jnp.where(source == anchor + 1.0, high, 0.0)

    def build(k, carry):
        cols = weigh(source, *taps(target_col, 0, k)).astype(jnp.bfloat16)
        blocks = [cols * masks[y] for y in range(tile)]
        for h in range(halves):
            anchor, low, high = taps(target_row[h], 1, k)
            low = jnp.where(same_column, low, 0.0).astype(jnp.bfloat16)
            high = jnp.where(same_column, high, 0.0).astype(jnp.bfloat16)
            after = (anchor + 1.0).astype(jnp.bfloat16)
            anchor = anchor.astype(jnp.bfloat16)
            for y in range(edge):
                span = pl.ds(y * edge, edge)
                line = jnp.full((), y, jnp.bfloat16)
                tab0[k, h, span, :] = blocks[y % tile] if y // tile == h else blank
                tab1[k, h, span, :] = jnp.where(anchor == line, low, jnp.where(after == line, high, blank))
        return carry

    lax.fori_loop(0, edge, build, 0)

    for copy in copies[: len(small)]:
        copy.wait()

    def splat(value):
        return jnp.full((SUB, LANES), value, jnp.float32)

    splats[EXT_SLOPE] = splat(egain[0] * LOG2E)
    splats[EXT_SHIFT] = splat(ebias[0] * LOG2E + math.log2(LOG2E))
    for c in range(3):
        splats[SLOPES + c] = splat(s_cgain[c] * 0.5)
        splats[SHIFTS + c] = splat(s_cbias[c] * 0.5)
    flips = []
    for v in range(2):
        flips.append(s_order[v, 0] > s_order[v, order.shape[1] - 1])
        splats[FLIPS + v] = splat(jnp.where(flips[v], 1.0, 0.0))
        rank = lax.bitwise_xor(me, s_order[v, 0])
        for bit in range(rounds):
            splats[FRONTS + v * rounds + bit] = splat(bit_of(rank, bit).astype(jnp.float32))

    for copy in ready[0]:
        copy.wait()
    for copy in copies[early:]:
        copy.start()
    for r in range(rows):
        to_slices(lines0, r, perm, moved)
    for k in range(edge):
        resample(k, 0, flips, moved, tab0, samples)

    total = v_cost.shape[1]
    here = lax.broadcasted_iota(jnp.int32, (chunk, total), 0)
    there = lax.broadcasted_iota(jnp.int32, (chunk, total), 1)
    row = v_cost[...].astype(jnp.float32)
    ones = jnp.ones((total, LANES), jnp.bfloat16)
    for i, quarter in enumerate(quarters):
        picked = jnp.where(here + quarter * chunk == there, row, 0.0).astype(jnp.bfloat16)
        levels[i] = jnp.dot(picked, ones, preferred_element_type=jnp.float32)

    mine = bit_of(me, 0)

    def item(v):
        return lambda i: shade(i, 1 - mine, low_bits, v, samples, levels.at[0], splats, send)

    count = chunk // SUB * halves // 2
    beside(2, count, edge, item(0), lambda k: resample(k, 1, flips, moved, tab1, samples))
    for copy in ready[1] + ready[2] + ready[3]:
        copy.wait()

    def slices(r):
        to_slices(lines1, r, perm, moved1)
        to_slices(lines2, r, perm, moved2)
        to_slices(lines3, r, perm, moved3)

    beside(2, count, rows, item(1), slices)


def second_kernel(low_bits, here0, here1, moved_next, tab0, levels, splats, kept, next0):
    mine = bit_of(lax.axis_index("depth"), 0)
    samples = (here0, here1)
    edge, halves, chunk, _ = here0.shape
    count = chunk // SUB * halves // 2
    flips = flips_of(splats)
    for v in range(2):
        beside(
            2, count, edge // 2,
            lambda i: shade(i, mine, low_bits, v, samples, levels.at[0], splats, kept),
            lambda k: resample(v * (edge // 2) + k, 0, flips, moved_next, tab0, (next0,)),
        )


def quarter_kernel(low_bits, index, levels, splats, here0, moved, tab1, *refs):
    if index < 3:
        moved_next, tab0, send, kept, next0, here1 = refs
    else:
        send, kept, here1 = refs
    samples = (here0, here1)
    mine = bit_of(lax.axis_index("depth"), 0)
    edge, halves, chunk, _ = here0.shape
    count = chunk // SUB * halves // 2
    flips = flips_of(splats)
    for v in range(2):

        def items(i):
            shade(i, 1 - mine, low_bits, v, samples, levels.at[index], splats, send)
            shade(i, mine, low_bits, v, samples, levels.at[index], splats, kept)

        def jobs(k):
            if v == 0:
                resample(k, 1, flips, moved, tab1, samples)
            else:
                resample(k, 0, flips, moved_next, tab0, (next0,))

        beside(4, count, edge if index < 3 or v == 0 else 0, items, jobs)


VMEM = pl.BlockSpec(memory_space=pltpu.VMEM)
HBM = pl.BlockSpec(memory_space=pltpu.HBM)


def call(kernel, ins, outs, cycles, scratch=(), limit=4 << 20, specs=None):
    outs = tuple(jax.ShapeDtypeStruct(shape, dtype) for shape, dtype in outs)
    return pl.pallas_call(
        kernel,
        out_shape=outs,
        in_specs=specs or [VMEM] * len(ins),
        out_specs=tuple(VMEM for _ in outs),
        scratch_shapes=list(scratch),
        compiler_params=pltpu.CompilerParams(vmem_limit_bytes=limit),
        cost_estimate=pl.CostEstimate(flops=cycles * 4096, bytes_accessed=1 << 18, transcendentals=0),
    )(*ins)


def render(rounds, low_bits, order, cgain, cbias, egain, ebias, cost, bricks):
    total, edge, plane = bricks.shape
    rows = total // BC // 4
    chunk, halves, size = rows * BC, plane // LANES, BC * edge
    f32, bf16 = jnp.float32, jnp.bfloat16
    part = ((rows * halves // 2, 2, 4, BC, LANES), f32)
    samples = ((edge, halves, chunk, LANES), f32)
    lines = ((rows, halves, BC, edge, LANES), bf16)
    moved = ((edge, halves, chunk, LANES), bf16)
    table = ((edge, halves, plane, LANES), bf16)
    square = ((size // LANES, size, LANES), bf16)
    levels = ((4, chunk, LANES), f32)
    splats = ((FRONTS + 2 * rounds, SUB, LANES), f32)
    bricks = bricks.reshape(total // BC, BC, edge, plane)
    far = lambda x: pltpu.with_memory_space_constraint(x, pltpu.HBM)
    ins = (far(order), far(cgain), far(cbias), egain, ebias, far(cost), far(bricks))
    specs = [HBM] * 3 + [pl.BlockSpec(memory_space=pltpu.SMEM)] * 2 + [HBM] * 2
    send0, *samples0, moved1, moved2, moved3, tab0, tab1, levels_, splats_ = call(
        functools.partial(first_kernel, rounds, low_bits), ins,
        (part, samples, samples, moved, moved, moved, table, table, levels, splats), 4000,
        [*[pltpu.VMEM(*lines)] * 4, pltpu.VMEM(*square), pltpu.VMEM(*moved),
         pltpu.SMEM(order.shape, order.dtype), pltpu.SMEM(cgain.shape, f32), pltpu.SMEM(cbias.shape, f32),
         pltpu.VMEM(cost.shape, cost.dtype), pltpu.SemaphoreType.DMA((4 + 4 * halves,))],
        20 << 20, specs,
    )
    kept0, samples1 = call(
        functools.partial(second_kernel, low_bits),
        (*samples0, moved1, tab0, levels_, splats_), (part, samples), 1800, (), 14 << 20,
    )
    scratch = [pltpu.VMEM(*samples)]
    send1, kept1, samples2 = call(
        functools.partial(quarter_kernel, low_bits, 1),
        (levels_, splats_, samples1, moved1, tab1, moved2, tab0), (part, part, samples), 3500, scratch, 14 << 20,
    )
    send2, kept2, samples3 = call(
        functools.partial(quarter_kernel, low_bits, 2),
        (levels_, splats_, samples2, moved2, tab1, moved3, tab0), (part, part, samples), 3500, scratch, 14 << 20,
    )
    send3, kept3 = call(
        functools.partial(quarter_kernel, low_bits, 3),
        (levels_, splats_, samples3, moved3, tab1), (part, part), 3300, scratch, 8 << 20,
    )
    return splats_, [(send0, kept0), (send1, kept1), (send2, kept2), (send3, kept3)]


def merged_pair(front, kept, incoming):
    behind = 1.0 - front * incoming[3]
    ahead = 1.0 - (1.0 - front) * kept[3]
    return [kept[c] * behind + incoming[c] * ahead for c in range(4)]


def front_of(splats, v, rounds, bit):
    one = splats[FRONTS + v * rounds + bit]
    return jnp.concatenate([one] * (BC // SUB), axis=0)


def read(ref, unit, v):
    parts = [ref[unit, v, c] for c in range(4)]
    return [decode(x) for x in parts] if ref.dtype == jnp.int16 else parts


def merge_kernel(rounds, bit, many, low_bits, splats, kept, *refs):
    incoming, outs = refs[:many], refs[many:]
    mine = bit_of(lax.axis_index("depth"), bit + many)
    units = kept.shape[0]
    for v in range(2):
        for i, out in enumerate(outs):
            for slot in range(units // len(outs)):
                unit = slot
                if len(outs) > 1:
                    unit = spread_bit(slot, low_bits, 1 - mine if i == 0 else mine)
                done = read(kept, unit, v)
                for n, came in enumerate(incoming):
                    done = merged_pair(front_of(splats, v, rounds, bit + n), done, read(came, unit, v))
                for c in range(4):
                    out[slot, v, c] = encode(done[c]) if out.dtype == jnp.int16 else done[c]


def merge(rounds, bit, low_bits, types, splats, kept, incoming):
    units, tail = kept.shape[0], kept.shape[1:]
    outs = tuple(((units // len(types), *tail), t) for t in types)
    kernel = functools.partial(merge_kernel, rounds, bit, len(incoming), low_bits)
    return call(kernel, (splats, kept, *incoming), outs, 300)


def finish_kernel(rounds, bit, edge, splats, kept, *refs):
    incoming, out = refs[:-1], refs[-1]
    chunks = LANES // edge
    chunk_of = lax.broadcasted_iota(jnp.int32, (SUB, LANES), 1) // edge
    for v in range(2):
        for unit in range(kept.shape[0]):
            done = read(kept, unit, v)
            for n, came in enumerate(incoming):
                done = merged_pair(front_of(splats, v, rounds, bit + n), done, read(came, unit, v))
            for c in range(4):
                for g in range(BC // SUB):
                    x = done[c][g * SUB : (g + 1) * SUB, :]
                    x = pltpu.roll(x, 0, 1, stride=edge, stride_axis=0)
                    for step in range(3):
                        turned = pltpu.roll(x, SUB - (1 << step), 0)
                        x = jnp.where(bit_of(chunk_of, step) == 1, turned, x)
                    x = pltpu.roll(x, 0, 1, stride=edge, stride_axis=0)
                    out[v, c, unit * chunks : (unit + 1) * chunks, g * LANES : (g + 1) * LANES] = x


def finish(rounds, bit, edge, splats, kept, incoming):
    units = kept.shape[0]
    out = ((2, 4, units * LANES // edge, BC * edge), jnp.float32)
    return call(functools.partial(finish_kernel, rounds, bit, edge), (splats, kept, *incoming), (out,), 1500)[0]


def swapped(x, bit):
    count = lax.axis_size("depth")
    return lax.ppermute(x, "depth", [(i, i ^ 1 << bit) for i in range(count)])


def shards(bricks, cost, order, color_gain, color_bias, ext_gain, ext_bias):
    bricks = bricks[0]
    total, edge, plane = bricks.shape
    count = lax.axis_size("depth")
    rounds = count.bit_length() - 1
    units = total // BC * (plane // LANES)
    low_bits = (units // count).bit_length() - 1
    splats, parts = render(
        rounds, low_bits, order, color_gain, color_bias, ext_gain, ext_bias, cost, bricks
    )
    f32, i16 = jnp.float32, jnp.int16
    near = rounds - 2

    def close(index):
        send, kept = parts[index]
        for bit in range(near - 1):
            incoming = swapped(send, bit)
            send, kept = merge(rounds, bit, low_bits, (f32, f32), splats, kept, [incoming])
        return kept, swapped(send, near - 1)

    def leave(index):
        kept, incoming = close(index)
        (done,) = merge(rounds, near - 1, low_bits, (i16,), splats, kept, [incoming])
        return swapped(done, near)

    far = leave(0)
    across = leave(1)
    kept, incoming = close(2)
    (done,) = merge(rounds, near - 1, low_bits, (i16,), splats, kept, [incoming, far])
    top = swapped(done, near + 1)
    kept, incoming = close(3)
    return finish(rounds, near - 1, edge, splats, kept, [incoming, across, top])


def solution(mesh):
    in_specs = (P("depth", "image", None, None), P("depth", "image"), P(), P(), P(), P(), P())
    out_specs = P(None, None, "depth", "image")

    return jax.shard_map(shards, mesh=mesh, in_specs=in_specs, out_specs=out_specs, check_vma=False)
```

```python
import functools
import math

import jax
import jax.numpy as jnp
from jax import lax
from jax.experimental import pallas as pl
from jax.experimental.pallas import tpu as pltpu
from jax.sharding import PartitionSpec as P


BC = 16
LANES = 128
SUB = 8
SHEAR = (0.45, -0.3)
LOG2E = 1.0 / math.log(2.0)

CODE_RANGE = 32.0
CODE_STEP = 2047.0
CODE_BIAS = 32768.0


def encode(x):
    logs = jnp.log(jnp.maximum(x, 2.0**-CODE_RANGE))
    code = logs * (CODE_STEP * LOG2E) + (CODE_RANGE * CODE_STEP + 0.5)
    return (code.astype(jnp.int32) - int(CODE_BIAS)).astype(jnp.int16)


def decode(code):
    value = code.astype(jnp.int32).astype(jnp.float32)
    return jnp.exp2(value * (1.0 / CODE_STEP) + (CODE_BIAS / CODE_STEP - CODE_RANGE))


EXT_SLOPE, EXT_SHIFT, SLOPES, SHIFTS, FLIPS, FRONTS = 0, 1, 2, 5, 8, 10


def bit_of(value, bit):
    return lax.bitwise_and(lax.shift_right_logical(value, bit), 1)


def spread_bit(slot, position, bit):
    high = lax.shift_left(lax.shift_right_logical(slot, position), position + 1)
    low = lax.bitwise_and(slot, (1 << position) - 1)
    return high + low + bit * (1 << position)


def shade(item, bit, low_bits, v, samples, levels, splats, out):
    edge, halves = samples[v].shape[0], samples[v].shape[1]
    slot, group = item // 2, lax.rem(item, 2)
    unit = spread_bit(slot, low_bits, bit)
    h = lax.rem(unit, halves)
    start = pl.multiple_of((unit // halves) * BC + group * SUB, SUB)
    level = levels[pl.ds(start, SUB), :]
    flip = splats[FLIPS + v]
    ext_slope, ext_shift = splats[EXT_SLOPE], splats[EXT_SHIFT]
    shift = []
    for j in range(4):
        need = j + flip * (3 - 2 * j)
        shift.append(jnp.where(level > need, ext_shift, -1e30))
    clear = jnp.ones((SUB, LANES), jnp.float32)
    depth = jnp.zeros((SUB, LANES), jnp.float32)
    sums = [jnp.zeros((SUB, LANES), jnp.float32) for _ in range(3)]
    for k in range(edge):
        s = samples[v][k, h, pl.ds(start, SUB), :]
        depth = depth - jnp.exp2(s * ext_slope + shift[k // (edge // 4)])
        beyond = jnp.exp2(depth)
        weight = clear - beyond
        clear = beyond
        for c in range(3):
            sums[c] = sums[c] + weight * jnp.tanh(s * splats[SLOPES + c] + splats[SHIFTS + c])
    opacity = 1.0 - clear
    place = pl.multiple_of(group * SUB, SUB)
    for c in range(3):
        out[slot, v, c, pl.ds(place, SUB), :] = (opacity + sums[c]) * 0.5
    out[slot, v, 3, pl.ds(place, SUB), :] = opacity


def wide(ref, *index):
    return jnp.concatenate([ref[(*index, h)] for h in range(ref.shape[len(index)])], axis=-1)


def to_slices(lines, r, perm, moved):
    edge, halves = moved.shape[0], moved.shape[1]
    x = jnp.concatenate([lines[r, h].reshape(BC * edge, LANES) for h in range(halves)], axis=-1)
    slices = jnp.dot(wide(perm), x, preferred_element_type=jnp.float32).astype(jnp.bfloat16)
    place = r * BC if isinstance(r, int) else pl.multiple_of(r * BC, BC)
    for k in range(edge):
        for h in range(halves):
            moved[k, h, pl.ds(place, BC), :] = slices[k * BC : (k + 1) * BC, h * LANES : (h + 1) * LANES]


def flips_of(splats):
    return [splats[FLIPS + v, 0, 0] > 0.5 for v in range(2)]


def resample(k, v, flips, moved, table, samples):
    edge, halves = samples[v].shape[0], samples[v].shape[1]
    result = jnp.dot(wide(moved, k), wide(table, k), preferred_element_type=jnp.float32)
    place = jnp.where(flips[v], edge - 1 - k, k)
    for h in range(halves):
        samples[v][place, h] = result[:, h * LANES : (h + 1) * LANES]


def beside(steps, items, jobs, item_fn, job_fn):
    def body(i, carry):
        for n in range(items // steps):
            item_fn(i * (items // steps) + n)
        for n in range(jobs // steps):
            job_fn(i * (jobs // steps) + n)
        return carry

    lax.fori_loop(0, steps, body, 0)


def first_kernel(
    rounds, low_bits,
    order, cgain, cbias, egain, ebias, cost, bricks,
    send, samples0, samples1, moved1, moved2, moved3, tab0, tab1, levels, splats,
    lines0, lines1, lines2, lines3, perm, moved, s_order, s_cgain, s_cbias, v_cost, sems,
):
    me = lax.axis_index("depth")
    rows, edge = lines0.shape[0], moved.shape[0]
    samples = (samples0, samples1)
    halves = samples0.shape[1]
    chunk = rows * BC
    top, second = bit_of(me, rounds - 1), bit_of(me, rounds - 2)
    quarters = [
        (1 - top) * 2 + 1 - second, (1 - top) * 2 + second, top * 2 + 1 - second, top * 2 + second
    ]
    small = [(order, s_order), (cgain, s_cgain), (cbias, s_cbias), (cost, v_cost)]
    pairs = list(small)
    for quarter, lines in zip(quarters, (lines0, lines1, lines2, lines3)):
        for h in range(halves):
            span = pl.ds(h * LANES, LANES)
            pairs.append((bricks.at[pl.ds(quarter * rows, rows), :, :, span], lines.at[:, h]))
    copies = [pltpu.make_async_copy(a, b, sems.at[i]) for i, (a, b) in enumerate(pairs)]
    early = len(small) + halves
    for copy in copies[:early]:
        copy.start()
    ready = [copies[len(small) + q * halves : len(small) + (q + 1) * halves] for q in range(4)]

    size = BC * edge
    for h in range(halves):
        out_row = lax.broadcasted_iota(jnp.int32, (size, LANES), 0)
        in_row = lax.broadcasted_iota(jnp.int32, (size, LANES), 1) + h * LANES
        wanted = lax.rem(out_row, BC) * edge + out_row // BC
        perm[h] = jnp.where(wanted == in_row, 1.0, 0.0).astype(jnp.bfloat16)

    tile = LANES // edge
    lane = lax.broadcasted_iota(jnp.int32, (edge, LANES), 1)
    source = lax.broadcasted_iota(jnp.int32, (edge, LANES), 0)
    masks = [jnp.where(lane // edge == (-y) % tile, 1.0, 0.0).astype(jnp.bfloat16) for y in range(tile)]
    same_column = lax.rem(lane, edge) == source
    blank = jnp.zeros((edge, LANES), jnp.bfloat16)
    target_col = lax.rem(lane, edge).astype(jnp.float32)
    target_row = [(lax.rem(tile - lane // edge, tile) + h * tile).astype(jnp.float32) for h in range(halves)]
    source = source.astype(jnp.float32)

    def taps(target, view, k):
        position = target + SHEAR[view] * (k.astype(jnp.float32) - (edge - 1) / 2.0)
        anchor = jnp.floor(position)
        high = position - anchor
        return anchor, 1.0 - high, high

    def weigh(source, anchor, low, high):
        return jnp.where(source == anchor, low, 0.0) + jnp.where(source == anchor + 1.0, high, 0.0)

    def build(k, carry):
        cols = weigh(source, *taps(target_col, 0, k)).astype(jnp.bfloat16)
        blocks = [cols * masks[y] for y in range(tile)]
        for h in range(halves):
            anchor, low, high = taps(target_row[h], 1, k)
            low = jnp.where(same_column, low, 0.0).astype(jnp.bfloat16)
            high = jnp.where(same_column, high, 0.0).astype(jnp.bfloat16)
            after = (anchor + 1.0).astype(jnp.bfloat16)
            anchor = anchor.astype(jnp.bfloat16)
            for y in range(edge):
                span = pl.ds(y * edge, edge)
                line = jnp.full((), y, jnp.bfloat16)
                tab0[k, h, span, :] = blocks[y % tile] if y // tile == h else blank
                tab1[k, h, span, :] = jnp.where(anchor == line, low, jnp.where(after == line, high, blank))
        return carry

    lax.fori_loop(0, edge, build, 0)

    for copy in copies[: len(small)]:
        copy.wait()

    def splat(value):
        return jnp.full((SUB, LANES), value, jnp.float32)

    splats[EXT_SLOPE] = splat(egain[0] * LOG2E)
    splats[EXT_SHIFT] = splat(ebias[0] * LOG2E + math.log2(LOG2E))
    for c in range(3):
        splats[SLOPES + c] = splat(s_cgain[c] * 0.5)
        splats[SHIFTS + c] = splat(s_cbias[c] * 0.5)
    flips = []
    for v in range(2):
        flips.append(s_order[v, 0] > s_order[v, order.shape[1] - 1])
        splats[FLIPS + v] = splat(jnp.where(flips[v], 1.0, 0.0))
        rank = lax.bitwise_xor(me, s_order[v, 0])
        for bit in range(rounds):
            splats[FRONTS + v * rounds + bit] = splat(bit_of(rank, bit).astype(jnp.float32))

    for copy in ready[0]:
        copy.wait()
    for copy in copies[early:]:
        copy.start()
    for r in range(rows):
        to_slices(lines0, r, perm, moved)
    for k in range(edge):
        resample(k, 0, flips, moved, tab0, samples)

    total = v_cost.shape[1]
    here = lax.broadcasted_iota(jnp.int32, (chunk, total), 0)
    there = lax.broadcasted_iota(jnp.int32, (chunk, total), 1)
    row = v_cost[...].astype(jnp.float32)
    ones = jnp.ones((total, LANES), jnp.bfloat16)
    for i, quarter in enumerate(quarters):
        picked = jnp.where(here + quarter * chunk == there, row, 0.0).astype(jnp.bfloat16)
        levels[i] = jnp.dot(picked, ones, preferred_element_type=jnp.float32)

    mine = bit_of(me, 0)

    def item(v):
        return lambda i: shade(i, 1 - mine, low_bits, v, samples, levels.at[0], splats, send)

    count = chunk // SUB * halves // 2
    beside(2, count, edge, item(0), lambda k: resample(k, 1, flips, moved, tab1, samples))
    for copy in ready[1] + ready[2] + ready[3]:
        copy.wait()

    def slices(r):
        to_slices(lines1, r, perm, moved1)
        to_slices(lines2, r, perm, moved2)
        to_slices(lines3, r, perm, moved3)

    beside(2, count, rows, item(1), slices)


def second_kernel(low_bits, here0, here1, moved_next, tab0, tab1, levels, splats, kept, next0, next1):
    mine = bit_of(lax.axis_index("depth"), 0)
    samples, samples_next = (here0, here1), (next0, next1)
    edge, halves, chunk, _ = here0.shape
    count = chunk // SUB * halves // 2
    flips = flips_of(splats)
    for v, table in enumerate((tab0, tab1)):
        beside(
            1, count, edge,
            lambda i: shade(i, mine, low_bits, v, samples, levels.at[0], splats, kept),
            lambda k: resample(k, v, flips, moved_next, table, samples_next),
        )


def quarter_kernel(low_bits, index, *refs):
    levels, splats, here0, here1, *refs = refs
    samples = (here0, here1)
    if index < 3:
        moved, tab0, tab1, send, kept, *samples_next = refs
    else:
        send, kept = refs
    mine = bit_of(lax.axis_index("depth"), 0)
    edge, halves, chunk, _ = here0.shape
    count = chunk // SUB * halves // 2
    rows = chunk // BC
    flips = flips_of(splats)
    for v in range(2):

        def items(i):
            shade(i, 1 - mine, low_bits, v, samples, levels.at[index], splats, send)
            shade(i, mine, low_bits, v, samples, levels.at[index], splats, kept)

        def jobs(r):
            for n in range(edge // rows):
                resample(r * (edge // rows) + n, v, flips, moved, tab1 if v else tab0, samples_next)

        beside(2, count, rows if index < 3 else 0, items, jobs)


VMEM = pl.BlockSpec(memory_space=pltpu.VMEM)
HBM = pl.BlockSpec(memory_space=pltpu.HBM)


def call(kernel, ins, outs, cycles, scratch=(), limit=4 << 20, specs=None):
    outs = tuple(jax.ShapeDtypeStruct(shape, dtype) for shape, dtype in outs)
    return pl.pallas_call(
        kernel,
        out_shape=outs,
        in_specs=specs or [VMEM] * len(ins),
        out_specs=tuple(VMEM for _ in outs),
        scratch_shapes=list(scratch),
        compiler_params=pltpu.CompilerParams(vmem_limit_bytes=limit),
        cost_estimate=pl.CostEstimate(flops=cycles * 4096, bytes_accessed=1 << 18, transcendentals=0),
    )(*ins)


def render(rounds, low_bits, order, cgain, cbias, egain, ebias, cost, bricks):
    total, edge, plane = bricks.shape
    rows = total // BC // 4
    chunk, halves, size = rows * BC, plane // LANES, BC * edge
    f32, bf16 = jnp.float32, jnp.bfloat16
    part = ((rows * halves // 2, 2, 4, BC, LANES), f32)
    samples = ((edge, halves, chunk, LANES), f32)
    lines = ((rows, halves, BC, edge, LANES), bf16)
    moved = ((edge, halves, chunk, LANES), bf16)
    table = ((edge, halves, plane, LANES), bf16)
    square = ((size // LANES, size, LANES), bf16)
    levels = ((4, chunk, LANES), f32)
    splats = ((FRONTS + 2 * rounds, SUB, LANES), f32)
    bricks = bricks.reshape(total // BC, BC, edge, plane)
    far = lambda x: pltpu.with_memory_space_constraint(x, pltpu.HBM)
    ins = (far(order), far(cgain), far(cbias), egain, ebias, far(cost), far(bricks))
    specs = [HBM] * 3 + [pl.BlockSpec(memory_space=pltpu.SMEM)] * 2 + [HBM] * 2
    send0, *samples0, moved1, moved2, moved3, tab0, tab1, levels_, splats_ = call(
        functools.partial(first_kernel, rounds, low_bits), ins,
        (part, samples, samples, moved, moved, moved, table, table, levels, splats), 4000,
        [*[pltpu.VMEM(*lines)] * 4, pltpu.VMEM(*square), pltpu.VMEM(*moved),
         pltpu.SMEM(order.shape, order.dtype), pltpu.SMEM(cgain.shape, f32), pltpu.SMEM(cbias.shape, f32),
         pltpu.VMEM(cost.shape, cost.dtype), pltpu.SemaphoreType.DMA((4 + 4 * halves,))],
        20 << 20, specs,
    )
    kept0, *samples1 = call(
        functools.partial(second_kernel, low_bits),
        (*samples0, moved1, tab0, tab1, levels_, splats_), (part, samples, samples), 1800, (), 14 << 20,
    )
    send1, kept1, *samples2 = call(
        functools.partial(quarter_kernel, low_bits, 1),
        (levels_, splats_, *samples1, moved2, tab0, tab1), (part, part, samples, samples), 3500, (), 14 << 20,
    )
    send2, kept2, *samples3 = call(
        functools.partial(quarter_kernel, low_bits, 2),
        (levels_, splats_, *samples2, moved3, tab0, tab1), (part, part, samples, samples), 3500, (), 14 << 20,
    )
    send3, kept3 = call(
        functools.partial(quarter_kernel, low_bits, 3),
        (levels_, splats_, *samples3), (part, part), 3300, (), 8 << 20,
    )
    return splats_, [(send0, kept0), (send1, kept1), (send2, kept2), (send3, kept3)]


def merged_pair(front, kept, incoming):
    behind = 1.0 - front * incoming[3]
    ahead = 1.0 - (1.0 - front) * kept[3]
    return [kept[c] * behind + incoming[c] * ahead for c in range(4)]


def front_of(splats, v, rounds, bit):
    one = splats[FRONTS + v * rounds + bit]
    return jnp.concatenate([one] * (BC // SUB), axis=0)


def read(ref, unit, v):
    parts = [ref[unit, v, c] for c in range(4)]
    return [decode(x) for x in parts] if ref.dtype == jnp.int16 else parts


def merge_kernel(rounds, bit, many, low_bits, splats, kept, *refs):
    incoming, outs = refs[:many], refs[many:]
    mine = bit_of(lax.axis_index("depth"), bit + many)
    units = kept.shape[0]
    for v in range(2):
        for i, out in enumerate(outs):
            for slot in range(units // len(outs)):
                unit = slot
                if len(outs) > 1:
                    unit = spread_bit(slot, low_bits, 1 - mine if i == 0 else mine)
                done = read(kept, unit, v)
                for n, came in enumerate(incoming):
                    done = merged_pair(front_of(splats, v, rounds, bit + n), done, read(came, unit, v))
                for c in range(4):
                    out[slot, v, c] = encode(done[c]) if out.dtype == jnp.int16 else done[c]


def merge(rounds, bit, low_bits, types, splats, kept, incoming):
    units, tail = kept.shape[0], kept.shape[1:]
    outs = tuple(((units // len(types), *tail), t) for t in types)
    kernel = functools.partial(merge_kernel, rounds, bit, len(incoming), low_bits)
    return call(kernel, (splats, kept, *incoming), outs, 300)


def finish_kernel(rounds, bit, edge, splats, kept, *refs):
    incoming, out = refs[:-1], refs[-1]
    chunks = LANES // edge
    chunk_of = lax.broadcasted_iota(jnp.int32, (SUB, LANES), 1) // edge
    for v in range(2):
        for unit in range(kept.shape[0]):
            done = read(kept, unit, v)
            for n, came in enumerate(incoming):
                done = merged_pair(front_of(splats, v, rounds, bit + n), done, read(came, unit, v))
            for c in range(4):
                for g in range(BC // SUB):
                    x = done[c][g * SUB : (g + 1) * SUB, :]
                    x = pltpu.roll(x, 0, 1, stride=edge, stride_axis=0)
                    for step in range(3):
                        turned = pltpu.roll(x, SUB - (1 << step), 0)
                        x = jnp.where(bit_of(chunk_of, step) == 1, turned, x)
                    x = pltpu.roll(x, 0, 1, stride=edge, stride_axis=0)
                    out[v, c, unit * chunks : (unit + 1) * chunks, g * LANES : (g + 1) * LANES] = x


def finish(rounds, bit, edge, splats, kept, incoming):
    units = kept.shape[0]
    out = ((2, 4, units * LANES // edge, BC * edge), jnp.float32)
    return call(functools.partial(finish_kernel, rounds, bit, edge), (splats, kept, *incoming), (out,), 1500)[0]


def swapped(x, bit):
    count = lax.axis_size("depth")
    return lax.ppermute(x, "depth", [(i, i ^ 1 << bit) for i in range(count)])


def shards(bricks, cost, order, color_gain, color_bias, ext_gain, ext_bias):
    bricks = bricks[0]
    total, edge, plane = bricks.shape
    count = lax.axis_size("depth")
    rounds = count.bit_length() - 1
    units = total // BC * (plane // LANES)
    low_bits = (units // count).bit_length() - 1
    splats, parts = render(
        rounds, low_bits, order, color_gain, color_bias, ext_gain, ext_bias, cost, bricks
    )
    f32, i16 = jnp.float32, jnp.int16
    near = rounds - 2

    def close(index):
        send, kept = parts[index]
        for bit in range(near - 1):
            incoming = swapped(send, bit)
            send, kept = merge(rounds, bit, low_bits, (f32, f32), splats, kept, [incoming])
        return kept, swapped(send, near - 1)

    def leave(index):
        kept, incoming = close(index)
        (done,) = merge(rounds, near - 1, low_bits, (i16,), splats, kept, [incoming])
        return swapped(done, near)

    across = leave(0)
    kept, incoming = close(1)
    (done,) = merge(rounds, near - 1, low_bits, (i16,), splats, kept, [incoming, across])
    top = swapped(done, near + 1)
    across = leave(2)
    kept, incoming = close(3)
    return finish(rounds, near - 1, edge, splats, kept, [incoming, across, top])


def solution(mesh):
    in_specs = (P("depth", "image", None, None), P("depth", "image"), P(), P(), P(), P(), P())
    out_specs = P(None, None, "depth", "image")

    return jax.shard_map(shards, mesh=mesh, in_specs=in_specs, out_specs=out_specs, check_vma=False)
```
